32 devices in a mesh: vox: 8 (over z, core), sta: 4 (over y, x).
Axes of the slice: x: 2, y: 2, z: 4, core: 2. Of those that a mesh axis runs over, the one named last changes fastest.
Arguments:
- green_tensor: bfloat16 [4, 6, 256, 1024], P('sta', None, None, 'vox'), may hold values from -0.078125 to 0.078125
- strain: bfloat16 [8, 6, 256, 1024], P('sta', None, None, 'vox'), may hold values from -6 to 6
- pair_events: int32 [4, 8], P('sta'), may hold values from -1 to 7, as said below
- pair_counts: int32 [4], P('sta'), may hold values from 6 to 8, as said below
- residuals: float32 [4, 8, 256], P('sta'), may hold values from -0.375 to 0.375
Outputs:
- kernel: float32 [1024], P(('vox', 'sta'))
The draws below stay inside these ranges and needn't reach their ends.
Inputs may be any that keep to these rules, and one draw needn't show every extreme that they name: `pair_events`: within a station the live entries are distinct earthquakes; slots at or beyond the station's count hold -1. `pair_counts`: some station has exactly 8 live slots in every draw.
All inputs are finite; a program needn't handle non-finite values.
Results may differ from the reference program's by a relative error of at most 0.0029.
Values may be sent and summed in bfloat16 or wider, within the bound.
A program may use at most 64 MiB of HBM per device.

```python
import jax
import jax.numpy as jnp
from jax import lax

COMP = 6
NT = 256
STATIONS = 4
EVENTS = 8
MAXP = 8
VOX = 1024


def pair_lists(key):
    first = jax.random.fold_in(key, 11)
    second = jax.random.fold_in(key, 12)
    third = jax.random.fold_in(key, 13)
    orders = jax.vmap(lambda k: jax.random.permutation(k, EVENTS))(jax.random.split(first, STATIONS))[:, :MAXP]
    drawn = jax.random.randint(second, (STATIONS,), 0, MAXP // 3 + 1)
    counts = MAXP - drawn
    busiest = jax.random.randint(third, (), 0, STATIONS)
    counts = jnp.where(jnp.arange(STATIONS) == busiest, MAXP, counts).astype(jnp.int32)
    places = jnp.arange(MAXP)[None, :]
    events = jnp.where(places < counts[:, None], orders, -1).astype(jnp.int32)
    return (events, counts)


def draw_pair_events(key, part):
    return pair_lists(key)[0]


def draw_pair_counts(key, part):
    return pair_lists(key)[1]


def shard_levels(own_key, shape, shards, smallest, top_value):
    factor_of = 1.0
    for dim, shards_of in shards:
        steps = jax.random.uniform(jax.random.fold_in(jax.random.fold_in(own_key, 6), dim), (shards_of,), jnp.float32, smallest / len(shards), top_value / len(shards))
        factor_of = factor_of * jnp.repeat(jnp.exp(steps), shape[dim] // shards_of).reshape((-1,) + (1,) * (len(shape) - 1 - dim))
    return factor_of


def noise(rng, shape, scale, bound, cuts=(), kind=jnp.bfloat16):
    array = scale * jax.random.normal(rng, shape, jnp.float32)
    if cuts:
        array = array * shard_levels(rng, shape, cuts, -0.22, 0.18)
    return jnp.clip(array, -bound, bound).astype(kind)


def setup_inputs(seed: int = 0) -> dict:
    arg_keys = jax.random.split(jax.random.key(seed), 6)
    return {
        "green_tensor": noise(arg_keys[0], (STATIONS, COMP, NT, VOX), (4 * COMP * NT) ** -0.5, 0.078125, ((0, 4), (3, 8))),
        "strain": noise(arg_keys[1], (EVENTS, COMP, NT, VOX), 1.0, 6.0, ((0, 4), (3, 8))),
        "pair_events": draw_pair_events(jax.random.fold_in(arg_keys[5], 71), 0),
        "pair_counts": draw_pair_counts(jax.random.fold_in(arg_keys[5], 71), 0),
        "residuals": noise(arg_keys[4], (STATIONS, MAXP, NT), NT ** -0.5, 0.375, ((0, 4),), jnp.float32),
    }


def toeplitz(wave):
    steps = jnp.arange(NT, dtype=jnp.int32)
    offset = steps[:, None] - steps[None, :]
    values = jnp.take(wave, jnp.clip(offset, 0, NT - 1), axis=-1)
    return jnp.where(offset >= 0, values, jnp.zeros_like(values))


def reference(green_tensor, strain, pair_events, pair_counts, residuals):
    def station(total, index):
        green = green_tensor[index].astype(jnp.float32)

        def slot(acc, place):
            event = pair_events[index, place]
            live = place < pair_counts[index]
            field = lax.dynamic_index_in_dim(strain, jnp.maximum(event, 0).astype(jnp.int32), 0, keepdims=False)
            matrix = toeplitz(residuals[index, place]).astype(jnp.bfloat16)
            conv = jnp.einsum("tu,cuv->ctv", matrix.astype(jnp.float32), field.astype(jnp.float32))
            term = jnp.sum(green * conv, axis=(0, 1))
            return acc + jnp.where(live, term, jnp.zeros_like(term)), None

        acc, _ = lax.scan(slot, total, jnp.arange(MAXP, dtype=jnp.int32))
        return acc, None

    start = jnp.zeros((VOX,), jnp.float32)
    kernel, _ = lax.scan(station, start, jnp.arange(STATIONS, dtype=jnp.int32))
    return kernel
```

```python
import functools

import jax
import jax.numpy as jnp
from jax import lax
from jax.experimental import pallas as pl
from jax.experimental.pallas import tpu as pltpu
from jax.sharding import PartitionSpec as P

LANES = 128
F32 = jnp.float32
BF16 = jnp.bfloat16


def kernel(
    n, events_ref, counts_ref, resid_ref, green_hbm, strain_hbm, out_ref,
    green, strain, packed_green, packed_strain, all_comb, all_green, all_strain, adjoint,
    load_sem, send_sem, recv_sem,
):
    me = lax.axis_index("sta")
    comps, nt, vox = green.shape
    local_events = strain.shape[0]
    slots = resid_ref.shape[0]
    width = vox // n
    per_tile = LANES // width
    full = comps // per_tile
    rest = comps % per_tile
    fit = min(per_tile // rest, local_events) if rest else 1
    blocks = nt // LANES

    def peer(d):
        pair = lax.rem(me // 2 + d // 2, n // 2)
        return 2 * pair + lax.rem(me + d, 2)

    order = list(range(n - 1, 0, -1))
    load_green = pltpu.make_async_copy(green_hbm.at[0], green, load_sem.at[0])
    load_strain = pltpu.make_async_copy(strain_hbm, strain, load_sem.at[1])
    load_green.start()
    load_strain.start()

    barrier = pltpu.get_barrier_semaphore()
    for d in order:
        pl.semaphore_signal(
            barrier, inc=1, device_id={"sta": peer(d)}, device_id_type=pl.DeviceIdType.MESH
        )

    def send(kind, src, dst, d):
        copy = pltpu.make_async_remote_copy(
            src_ref=src,
            dst_ref=dst.at[me],
            send_sem=send_sem.at[kind, d],
            recv_sem=recv_sem.at[kind, me],
            device_id={"sta": peer(d)},
            device_id_type=pl.DeviceIdType.MESH,
        )
        copy.start()
        return copy

    def wait_from(kind, dst, j):
        pltpu.make_async_remote_copy(
            src_ref=dst.at[j],
            dst_ref=dst.at[j],
            send_sem=send_sem.at[kind, 0],
            recv_sem=recv_sem.at[kind, j],
            device_id={"sta": j},
            device_id_type=pl.DeviceIdType.MESH,
        ).wait_recv()

    rows = lax.broadcasted_iota(jnp.int32, (all_comb.shape[1], nt), 0)
    comb = jnp.zeros((all_comb.shape[1], nt), F32)
    for p in range(slots):
        event = jnp.where(p < counts_ref[0], events_ref[0, p], -1)
        comb = comb + jnp.where(rows == event, resid_ref[p : p + 1, :], 0.0)
    all_comb[me] = comb

    lane = lax.broadcasted_iota(jnp.int32, (LANES, LANES), 0)
    column = lax.broadcasted_iota(jnp.int32, (LANES, LANES), 1)

    def pick(j, slot):
        inside = (column >= slot * width) & (column < (slot + 1) * width)
        return inside & (lane == column + (j - slot) * width)

    def as_matrix(masks):
        return jnp.concatenate([jnp.where(m, 1.0, 0.0).astype(BF16) for m in masks], axis=0)

    def gathered(tiles, matrix):
        wide = jnp.concatenate(tiles, axis=1)
        return jnp.dot(wide, matrix[: len(tiles) * LANES], preferred_element_type=F32).astype(BF16)

    def pack_green(j, masks, matrix, dst, index):
        for a in range(full):
            dst[index, a] = gathered([green[a * per_tile + k] for k in range(per_tile)], matrix)
        if rest:
            repeated = []
            for k in range(rest):
                hit = masks[k]
                for i in range(1, fit):
                    hit = hit | masks[i * rest + k]
                repeated.append(hit)
            dst[index, full] = gathered(
                [green[full * per_tile + k] for k in range(rest)], as_matrix(repeated)
            )

    def pack_strain(matrix, dst, index):
        tile = 0
        for e in range(local_events):
            for a in range(full):
                dst[index, tile] = gathered(
                    [strain[e, a * per_tile + k] for k in range(per_tile)], matrix
                )
                tile += 1
        if rest:
            for e in range(0, local_events, fit):
                dst[index, tile] = gathered(
                    [strain[e + i, full * per_tile + k] for i in range(fit) for k in range(rest)],
                    matrix,
                )
                tile += 1

    matrices = {}
    for d in order + [0]:
        j = peer(d)
        masks = [pick(j, slot) for slot in range(per_tile)]
        matrices[d] = (j, masks, as_matrix(masks))

    load_green.wait()
    copies = []
    pl.semaphore_wait(barrier, n - 1)
    for d in order:
        copies.append(send(0, all_comb.at[me], all_comb, d))
    waiting = None
    for d in order:
        pack_green(*matrices[d], packed_green, d)
        if waiting is not None:
            copies.append(send(1, packed_green.at[waiting], all_green, waiting))
        waiting = d
    pack_green(*matrices[0], all_green, me)
    copies.append(send(1, packed_green.at[waiting], all_green, waiting))
    load_strain.wait()
    waiting = None
    for d in order:
        pack_strain(matrices[d][2], packed_strain, d)
        if waiting is not None:
            copies.append(send(2, packed_strain.at[waiting], all_strain, waiting))
        waiting = d
    pack_strain(matrices[0][2], all_strain, me)
    copies.append(send(2, packed_strain.at[waiting], all_strain, waiting))

    for d in order:
        wait_from(0, all_comb, peer(d))
    for d in order:
        wait_from(1, all_green, peer(d))

    later = column >= lane
    nothing = jnp.zeros((LANES, LANES), BF16)
    tiles = all_green.shape[1]

    @pl.loop(0, all_comb.shape[1])
    def _(e):
        total = jnp.zeros((nt, tiles * LANES), F32)
        for s in range(n):
            wave = all_comb[s, pl.ds(e, 1), :]
            turned = []
            for k in range(blocks):
                piece = jnp.broadcast_to(wave[:, k * LANES : (k + 1) * LANES], (LANES, LANES))
                turned.append(pltpu.roll(piece, 0, 1, stride=1, stride_axis=0))
            diag = [
                jnp.where(later, turned[k], turned[k - 1] if k else 0.0).astype(BF16)
                for k in range(blocks)
            ]
            matrix = jnp.concatenate(
                [
                    jnp.concatenate([nothing] * i + diag[: blocks - i], axis=1)
                    for i in range(blocks)
                ],
                axis=0,
            )
            field = jnp.concatenate([all_green[s, t] for t in range(tiles)], axis=1)
            total = total + jnp.dot(matrix, field, preferred_element_type=F32)
        adjoint[e] = total

    spot = lax.broadcasted_iota(jnp.int32, (nt, LANES), 1)

    def meet(j):
        part = jnp.zeros((1, LANES), F32)
        tile = 0
        for e in range(local_events):
            for a in range(full):
                field = all_strain[j, tile].astype(F32)
                one = adjoint[j * local_events + e, :, a * LANES : (a + 1) * LANES]
                part = part + jnp.sum(field * one, axis=0, keepdims=True)
                tile += 1
        if rest:
            for e in range(0, local_events, fit):
                field = all_strain[j, tile].astype(F32)
                one = adjoint[j * local_events + e, :, full * LANES :]
                for i in range(1, fit):
                    other = adjoint[j * local_events + e + i, :, full * LANES :]
                    one = jnp.where(spot < i * rest * width, one, other)
                part = part + jnp.sum(
                    jnp.where(spot < fit * rest * width, field * one, 0.0), axis=0, keepdims=True
                )
                tile += 1
        return part

    answer = meet(me)
    for d in order:
        j = peer(d)
        wait_from(2, all_strain, j)
        answer = answer + meet(j)
    total = answer[:, :width]
    for k in range(1, per_tile):
        total = total + answer[:, k * width : (k + 1) * width]
    out_ref[...] = total[0]
    for copy in copies:
        copy.wait_send()


def square_kernel(
    events_hbm, counts_hbm, resid_hbm, green_hbm, strain_hbm, out_ref,
    events_ref, counts_ref, resid, own_head, far_head, own_field, far_field, raw_green, raw_strain,
    send_tail, own_tail, far_tail, send_bits, own_bits, far_bits, waves, toeplitz, own_wide, far_wide,
    early, head_sum, tail_sum, load_sem, send_sem, recv_sem,
):
    me = lax.axis_index("sta")
    x, y = lax.rem(me, 2), me // 2
    odd = lax.rem(x + y, 2)
    beside = me + 1 - 2 * x
    above = lax.rem(me + 2, 4)
    first = beside + odd * (above - beside)
    second = above + odd * (beside - above)
    across = 3 - me
    rest, nt, vox = raw_green.shape
    local_events = raw_strain.shape[0]
    events = waves.shape[1]
    width = vox // 4
    per_tile = LANES // width
    half = nt // 2

    barrier = pltpu.get_barrier_semaphore()
    for target in (first, second):
        pl.semaphore_signal(
            barrier, inc=1, device_id={"sta": target}, device_id_type=pl.DeviceIdType.MESH
        )

    loads = {}
    for name, src, dst in (
        ("events", events_hbm, events_ref),
        ("counts", counts_hbm, counts_ref),
        ("resid", resid_hbm, resid),
        ("green", green_hbm.at[0, pl.ds(4, rest)], raw_green),
        ("strain", strain_hbm.at[:, pl.ds(4, rest)], raw_strain),
        ("own_head", green_hbm.at[0, me], own_head.at[0]),
        ("far_head", green_hbm.at[0, first], far_head.at[0]),
        ("own_field", strain_hbm.at[:, me], own_field.at[0]),
        ("far_field", strain_hbm.at[:, first], far_field.at[0]),
    ):
        loads[name] = pltpu.make_async_copy(src, dst, load_sem.at[len(loads)])
        loads[name].start()

    plan = {}
    for name, src, dst, target in (
        ("u0h", green_hbm.at[0, across], far_head.at[2], first),
        ("u2h", green_hbm.at[0, first], own_head.at[2], first),
        ("u1h", strain_hbm.at[:, across], far_field.at[1], first),
        ("u3h", far_head.at[2], own_head.at[3], first),
        ("w1h", green_hbm.at[0, second], own_head.at[1], second),
        ("w0h", green_hbm.at[0, me], far_head.at[1], second),
        ("w2h", strain_hbm.at[:, second], own_field.at[1], second),
        ("w4h", own_head.at[1], far_head.at[3], second),
        ("wave1", waves.at[0], waves.at[2], first),
        ("wave2", waves.at[0], waves.at[1], second),
        ("wave3", waves.at[2], waves.at[3], first),
        ("u0t", send_tail.at[0], far_tail.at[2], first),
        ("u2t", far_tail.at[0], own_tail.at[2], first),
        ("u1t", send_bits.at[0], far_bits.at[1], first),
        ("u3t", far_tail.at[2], own_tail.at[3], first),
        ("w1t", send_tail.at[1], own_tail.at[1], second),
        ("w0t", own_tail.at[0], far_tail.at[1], second),
        ("w2t", send_bits.at[1], own_bits.at[1], second),
        ("w4t", own_tail.at[1], far_tail.at[3], second),
        ("head1", head_sum.at[0], head_sum.at[2], first),
        ("head2", head_sum.at[0], head_sum.at[1], second),
        ("head3", head_sum.at[0], head_sum.at[3], across),
        ("tail", tail_sum.at[0], tail_sum.at[1], first),
    ):
        plan[name] = pltpu.make_async_remote_copy(
            src_ref=src,
            dst_ref=dst,
            send_sem=send_sem.at[len(plan)],
            recv_sem=recv_sem.at[len(plan)],
            device_id={"sta": target},
            device_id_type=pl.DeviceIdType.MESH,
        )

    lane = lax.broadcasted_iota(jnp.int32, (LANES, LANES), 0)
    column = lax.broadcasted_iota(jnp.int32, (LANES, LANES), 1)
    later = column >= lane
    low = column < LANES // 2

    def picker(j):
        parts = []
        for slot in range(per_tile):
            inside = (column >= slot * width) & (column < (slot + 1) * width)
            hit = inside & (lane == column + (j - slot) * width)
            parts.append(jnp.where(hit, 1.0, 0.0).astype(BF16))
        return jnp.concatenate(parts, axis=0)

    def folded(source, matrix):
        wide = jnp.concatenate(
            [source[k, h * half : (h + 1) * half] for h in range(2) for k in range(rest)], axis=1
        )
        return jnp.dot(wide, matrix, preferred_element_type=F32).astype(BF16)

    def make_toeplitz(s):
        @pl.loop(0, 3 * local_events)
        def _(k):
            group = k // local_events
            owner = me + (group % 2) * (first - me) + (group // 2) * (second - me)
            wave = waves[s, pl.ds(owner * local_events + k - group * local_events, 1), :]
            before = 0.0
            for b in range(2):
                piece = jnp.broadcast_to(wave[:, b * LANES : (b + 1) * LANES], (LANES, LANES))
                turned = pltpu.roll(piece, 0, 1, stride=1, stride_axis=0)
                toeplitz[k, s, b] = jnp.where(later, turned, before).astype(BF16)
                before = turned

    def widen(source, s, dst):
        piece = source[s].astype(F32)
        dst[s, :half] = source[s]
        dst[s, half:] = jnp.where(low, pltpu.roll(piece, LANES // 2, 1), 0.0).astype(BF16)

    to_across, to_second, to_me, to_first = (picker(j) for j in (across, second, me, first))

    pl.semaphore_wait(barrier, 2)
    for name in ("u0h", "w1h", "u2h", "w0h"):
        plan[name].start()

    for name in ("events", "counts", "resid"):
        loads[name].wait()
    rows = lax.broadcasted_iota(jnp.int32, (events, nt), 0)
    comb = jnp.zeros((events, nt), F32)
    for p in range(resid.shape[1]):
        event = jnp.where(p < counts_ref[0], events_ref[0, p], -1)
        comb = comb + jnp.where(rows == event, resid[0, p : p + 1, :], 0.0)
    waves[0] = comb

    loads["green"].wait()
    send_tail[0] = folded(raw_green, to_across)
    send_tail[1] = folded(raw_green, to_second)
    for name in ("wave1", "wave2", "u0t", "w1t", "u1h", "w2h"):
        plan[name].start()
    far_tail[0] = folded(raw_green, to_first)
    own_tail[0] = folded(raw_green, to_me)
    loads["strain"].wait()
    for e in range(local_events):
        send_bits[0, e] = folded(raw_strain.at[e], to_across)
        send_bits[1, e] = folded(raw_strain.at[e], to_second)
    make_toeplitz(0)
    plan["u0h"].wait_recv()
    plan["u3h"].start()
    plan["w1h"].wait_recv()
    plan["w4h"].start()
    plan["wave1"].wait_recv()
    plan["wave3"].start()
    for name in ("u1t", "w0t", "u2t"):
        plan[name].start()
    for e in range(local_events):
        far_bits[0, e] = folded(raw_strain.at[e], to_first)
        own_bits[0, e] = folded(raw_strain.at[e], to_me)
    make_toeplitz(2)
    plan["wave2"].wait_recv()
    make_toeplitz(1)
    plan["u0t"].wait_recv()
    plan["u3t"].start()
    plan["w1t"].wait_recv()
    plan["w4t"].start()
    plan["w2t"].start()
    plan["wave3"].wait_recv()
    make_toeplitz(3)
    for s in range(3):
        if s < 2:
            widen(own_tail, s, own_wide)
        if s != 1:
            widen(far_tail, s, far_wide)

    def head_matrix(k):
        nothing = jnp.zeros((half, half), BF16)
        top = [toeplitz[k, s, b] for s in range(4) for b in range(2)]
        bottom = [piece for s in range(4) for piece in (nothing, toeplitz[k, s, 0])]
        return jnp.concatenate(
            [jnp.concatenate(top, axis=1), jnp.concatenate(bottom, axis=1)], axis=0
        )

    def tail_matrix(k, stations):
        return jnp.concatenate([toeplitz[k, s, b] for s in stations for b in range(2)], axis=1)

    def met(field, adjoint):
        return jnp.sum(field.astype(F32) * adjoint, axis=0, keepdims=True)

    for name in ("own_head", "far_head", "own_field", "far_field"):
        loads[name].wait()
    for name in ("u2h", "w0h", "u1h", "w2h", "u3h", "w4h"):
        plan[name].wait_recv()
    own_stack = jnp.concatenate([own_head[s] for s in range(4)], axis=0)
    far_stack = jnp.concatenate([far_head[s] for s in range(4)], axis=0)
    both_stack = jnp.concatenate([own_stack, far_stack], axis=1)
    part = jnp.zeros((1, LANES), F32)
    for e in range(local_events):
        both = jnp.dot(head_matrix(e), both_stack, preferred_element_type=F32)
        part = part + met(own_field[0, e], both[:, :LANES]) + met(far_field[0, e], both[:, LANES:])
        one = jnp.dot(head_matrix(local_events + e), own_stack, preferred_element_type=F32)
        part = part + met(own_field[1, e], one)
        one = jnp.dot(head_matrix(2 * local_events + e), far_stack, preferred_element_type=F32)
        part = part + met(far_field[1, e], one)
    head_sum[0] = part
    for name in ("head3", "head1", "head2"):
        plan[name].start()

    for name in ("w0t", "u1t", "w4t"):
        plan[name].wait_recv()
    widen(far_tail, 1, far_wide)
    widen(far_tail, 3, far_wide)
    far_rhs = jnp.concatenate([far_wide[s] for s in range(4)], axis=0)
    part = jnp.zeros((1, LANES), F32)
    for g, side in ((0, 0), (2, 1)):
        for e in range(local_events):
            k = g * local_events + e
            one = jnp.dot(tail_matrix(k, range(4)), far_rhs, preferred_element_type=F32)
            part = part + met(far_bits[side, e], one)
    tail_sum[0] = part
    plan["tail"].start()

    plan["u2t"].wait_recv()
    widen(own_tail, 2, own_wide)
    own_rhs = jnp.concatenate([own_wide[s] for s in range(3)], axis=0)
    for k in range(2 * local_events):
        early[k] = jnp.dot(tail_matrix(k, range(3)), own_rhs, preferred_element_type=F32)
    plan["u3t"].wait_recv()
    widen(own_tail, 3, own_wide)
    plan["w2t"].wait_recv()
    part = jnp.zeros((1, LANES), F32)
    for g in range(2):
        for e in range(local_events):
            k = g * local_events + e
            one = early[k] + jnp.dot(
                tail_matrix(k, (3,)), own_wide[3], preferred_element_type=F32
            )
            part = part + met(own_bits[g, e], one)
    for name in ("head1", "head2", "head3", "tail"):
        plan[name].wait_recv()
    heads = head_sum[0] + head_sum[1] + head_sum[2] + head_sum[3]
    spot = lax.broadcasted_iota(jnp.int32, (1, LANES), 1)
    mine = (spot >= me * width) & (spot < (me + 1) * width)
    answer = part + tail_sum[1] + jnp.where(mine, heads, 0.0)
    total = answer[:, :width]
    for k in range(1, per_tile):
        total = total + answer[:, k * width : (k + 1) * width]
    out_ref[...] = total[0]
    for copy in plan.values():
        copy.wait_send()


def solution(mesh):
    n = mesh.shape["sta"]

    def body(green_tensor, strain, pair_events, pair_counts, residuals):
        _, comps, nt, vox = green_tensor.shape
        local_events = strain.shape[0]
        width = vox // n
        per_tile = LANES // width
        full = comps // per_tile
        rest = comps % per_tile
        fit = min(per_tile // rest, local_events) if rest else 1
        green_tiles = full + (1 if rest else 0)
        strain_tiles = full * local_events + (local_events // fit if rest else 0)
        events = n * local_events
        pairs = pair_events.shape[1]
        left = comps - n
        square = n == 4 and nt == 2 * LANES and 0 < left and 2 * left == per_tile
        if square:
            steps = square_kernel
            half = nt // 2
            head = (4, nt, LANES)
            field = (2, local_events, nt, LANES)
            tail = (4, half, LANES)
            bits = (2, local_events, half, LANES)
            scratch = [
                pltpu.SMEM((1, pairs), jnp.int32),
                pltpu.SMEM((1,), jnp.int32),
                pltpu.VMEM((1, pairs, nt), F32),
                pltpu.VMEM(head, BF16),
                pltpu.VMEM(head, BF16),
                pltpu.VMEM(field, BF16),
                pltpu.VMEM(field, BF16),
                pltpu.VMEM((left, nt, vox), BF16),
                pltpu.VMEM((local_events, left, nt, vox), BF16),
                pltpu.VMEM((2, half, LANES), BF16),
                pltpu.VMEM(tail, BF16),
                pltpu.VMEM(tail, BF16),
                pltpu.VMEM(bits, BF16),
                pltpu.VMEM(bits, BF16),
                pltpu.VMEM(bits, BF16),
                pltpu.VMEM((4, events, nt), F32),
                pltpu.VMEM((3 * local_events, 4, 2, half, half), BF16),
                pltpu.VMEM(head, BF16),
                pltpu.VMEM(head, BF16),
                pltpu.VMEM((2 * local_events, half, LANES), F32),
                pltpu.VMEM((4, 1, LANES), F32),
                pltpu.VMEM((2, 1, LANES), F32),
                pltpu.SemaphoreType.DMA((9,)),
                pltpu.SemaphoreType.DMA((23,)),
                pltpu.SemaphoreType.DMA((23,)),
            ]
        else:
            steps = functools.partial(kernel, n)
            scratch = [
                pltpu.VMEM((comps, nt, vox), BF16),
                pltpu.VMEM((local_events, comps, nt, vox), BF16),
                pltpu.VMEM((n, green_tiles, nt, LANES), BF16),
                pltpu.VMEM((n, strain_tiles, nt, LANES), BF16),
                pltpu.VMEM((n, events, nt), F32),
                pltpu.VMEM((n, green_tiles, nt, LANES), BF16),
                pltpu.VMEM((n, strain_tiles, nt, LANES), BF16),
                pltpu.VMEM((events, nt, green_tiles * LANES), F32),
                pltpu.SemaphoreType.DMA((2,)),
                pltpu.SemaphoreType.DMA((3, n)),
                pltpu.SemaphoreType.DMA((3, n)),
            ]
        if square:
            return pl.pallas_call(
                steps,
                out_shape=pltpu.VMEM((width,), F32),
                in_specs=[pl.BlockSpec(memory_space=pl.ANY)] * 5,
                out_specs=pl.BlockSpec(memory_space=pltpu.VMEM),
                scratch_shapes=scratch,
                compiler_params=pltpu.CompilerParams(collective_id=0, has_side_effects=True),
            )(pair_events, pair_counts, residuals, green_tensor, strain)
        return pl.pallas_call(
            steps,
            out_shape=jax.ShapeDtypeStruct((width,), F32),
            in_specs=[
                pl.BlockSpec(memory_space=pltpu.SMEM),
                pl.BlockSpec(memory_space=pltpu.SMEM),
                pl.BlockSpec(memory_space=pltpu.VMEM),
                pl.BlockSpec(memory_space=pl.ANY),
                pl.BlockSpec(memory_space=pl.ANY),
            ],
            out_specs=pl.BlockSpec(memory_space=pltpu.VMEM),
            scratch_shapes=scratch,
            compiler_params=pltpu.CompilerParams(collective_id=0, has_side_effects=True),
        )(pair_events, pair_counts, residuals[0], green_tensor, strain)

    in_specs = (
        P("sta", None, None, "vox"),
        P("sta", None, None, "vox"),
        P("sta", None),
        P("sta"),
        P("sta", None, None),
    )
    out_specs = P(("vox", "sta"))
    return jax.shard_map(body, mesh=mesh, in_specs=in_specs, out_specs=out_specs, check_vma=False)
```

```python
import functools

import jax
import jax.numpy as jnp
from jax import lax
from jax.experimental import pallas as pl
from jax.experimental.pallas import tpu as pltpu
from jax.sharding import PartitionSpec as P

LANES = 128
F32 = jnp.float32
BF16 = jnp.bfloat16


def kernel(
    n, events_ref, counts_ref, resid_ref, green_hbm, strain_hbm, out_ref,
    green, strain, packed_green, packed_strain, all_comb, all_green, all_strain, adjoint,
    load_sem, send_sem, recv_sem,
):
    me = lax.axis_index("sta")
    comps, nt, vox = green.shape
    local_events = strain.shape[0]
    slots = resid_ref.shape[0]
    width = vox // n
    per_tile = LANES // width
    full = comps // per_tile
    rest = comps % per_tile
    fit = min(per_tile // rest, local_events) if rest else 1
    blocks = nt // LANES

    def peer(d):
        pair = lax.rem(me // 2 + d // 2, n // 2)
        return 2 * pair + lax.rem(me + d, 2)

    order = list(range(n - 1, 0, -1))
    load_green = pltpu.make_async_copy(green_hbm.at[0], green, load_sem.at[0])
    load_strain = pltpu.make_async_copy(strain_hbm, strain, load_sem.at[1])
    load_green.start()
    load_strain.start()

    barrier = pltpu.get_barrier_semaphore()
    for d in order:
        pl.semaphore_signal(
            barrier, inc=1, device_id={"sta": peer(d)}, device_id_type=pl.DeviceIdType.MESH
        )

    def send(kind, src, dst, d):
        copy = pltpu.make_async_remote_copy(
            src_ref=src,
            dst_ref=dst.at[me],
            send_sem=send_sem.at[kind, d],
            recv_sem=recv_sem.at[kind, me],
            device_id={"sta": peer(d)},
            device_id_type=pl.DeviceIdType.MESH,
        )
        copy.start()
        return copy

    def wait_from(kind, dst, j):
        pltpu.make_async_remote_copy(
            src_ref=dst.at[j],
            dst_ref=dst.at[j],
            send_sem=send_sem.at[kind, 0],
            recv_sem=recv_sem.at[kind, j],
            device_id={"sta": j},
            device_id_type=pl.DeviceIdType.MESH,
        ).wait_recv()

    rows = lax.broadcasted_iota(jnp.int32, (all_comb.shape[1], nt), 0)
    comb = jnp.zeros((all_comb.shape[1], nt), F32)
    for p in range(slots):
        event = jnp.where(p < counts_ref[0], events_ref[0, p], -1)
        comb = comb + jnp.where(rows == event, resid_ref[p : p + 1, :], 0.0)
    all_comb[me] = comb

    lane = lax.broadcasted_iota(jnp.int32, (LANES, LANES), 0)
    column = lax.broadcasted_iota(jnp.int32, (LANES, LANES), 1)

    def pick(j, slot):
        inside = (column >= slot * width) & (column < (slot + 1) * width)
        return inside & (lane == column + (j - slot) * width)

    def as_matrix(masks):
        return jnp.concatenate([jnp.where(m, 1.0, 0.0).astype(BF16) for m in masks], axis=0)

    def gathered(tiles, matrix):
        wide = jnp.concatenate(tiles, axis=1)
        return jnp.dot(wide, matrix[: len(tiles) * LANES], preferred_element_type=F32).astype(BF16)

    def pack_green(j, masks, matrix, dst, index):
        for a in range(full):
            dst[index, a] = gathered([green[a * per_tile + k] for k in range(per_tile)], matrix)
        if rest:
            repeated = []
            for k in range(rest):
                hit = masks[k]
                for i in range(1, fit):
                    hit = hit | masks[i * rest + k]
                repeated.append(hit)
            dst[index, full] = gathered(
                [green[full * per_tile + k] for k in range(rest)], as_matrix(repeated)
            )

    def pack_strain(matrix, dst, index):
        tile = 0
        for e in range(local_events):
            for a in range(full):
                dst[index, tile] = gathered(
                    [strain[e, a * per_tile + k] for k in range(per_tile)], matrix
                )
                tile += 1
        if rest:
            for e in range(0, local_events, fit):
                dst[index, tile] = gathered(
                    [strain[e + i, full * per_tile + k] for i in range(fit) for k in range(rest)],
                    matrix,
                )
                tile += 1

    matrices = {}
    for d in order + [0]:
        j = peer(d)
        masks = [pick(j, slot) for slot in range(per_tile)]
        matrices[d] = (j, masks, as_matrix(masks))

    load_green.wait()
    copies = []
    pl.semaphore_wait(barrier, n - 1)
    for d in order:
        copies.append(send(0, all_comb.at[me], all_comb, d))
    waiting = None
    for d in order:
        pack_green(*matrices[d], packed_green, d)
        if waiting is not None:
            copies.append(send(1, packed_green.at[waiting], all_green, waiting))
        waiting = d
    pack_green(*matrices[0], all_green, me)
    copies.append(send(1, packed_green.at[waiting], all_green, waiting))
    load_strain.wait()
    waiting = None
    for d in order:
        pack_strain(matrices[d][2], packed_strain, d)
        if waiting is not None:
            copies.append(send(2, packed_strain.at[waiting], all_strain, waiting))
        waiting = d
    pack_strain(matrices[0][2], all_strain, me)
    copies.append(send(2, packed_strain.at[waiting], all_strain, waiting))

    for d in order:
        wait_from(0, all_comb, peer(d))
    for d in order:
        wait_from(1, all_green, peer(d))

    later = column >= lane
    nothing = jnp.zeros((LANES, LANES), BF16)
    tiles = all_green.shape[1]

    @pl.loop(0, all_comb.shape[1])
    def _(e):
        total = jnp.zeros((nt, tiles * LANES), F32)
        for s in range(n):
            wave = all_comb[s, pl.ds(e, 1), :]
            turned = []
            for k in range(blocks):
                piece = jnp.broadcast_to(wave[:, k * LANES : (k + 1) * LANES], (LANES, LANES))
                turned.append(pltpu.roll(piece, 0, 1, stride=1, stride_axis=0))
            diag = [
                jnp.where(later, turned[k], turned[k - 1] if k else 0.0).astype(BF16)
                for k in range(blocks)
            ]
            matrix = jnp.concatenate(
                [
                    jnp.concatenate([nothing] * i + diag[: blocks - i], axis=1)
                    for i in range(blocks)
                ],
                axis=0,
            )
            field = jnp.concatenate([all_green[s, t] for t in range(tiles)], axis=1)
            total = total + jnp.dot(matrix, field, preferred_element_type=F32)
        adjoint[e] = total

    spot = lax.broadcasted_iota(jnp.int32, (nt, LANES), 1)

    def meet(j):
        part = jnp.zeros((1, LANES), F32)
        tile = 0
        for e in range(local_events):
            for a in range(full):
                field = all_strain[j, tile].astype(F32)
                one = adjoint[j * local_events + e, :, a * LANES : (a + 1) * LANES]
                part = part + jnp.sum(field * one, axis=0, keepdims=True)
                tile += 1
        if rest:
            for e in range(0, local_events, fit):
                field = all_strain[j, tile].astype(F32)
                one = adjoint[j * local_events + e, :, full * LANES :]
                for i in range(1, fit):
                    other = adjoint[j * local_events + e + i, :, full * LANES :]
                    one = jnp.where(spot < i * rest * width, one, other)
                part = part + jnp.sum(
                    jnp.where(spot < fit * rest * width, field * one, 0.0), axis=0, keepdims=True
                )
                tile += 1
        return part

    answer = meet(me)
    for d in order:
        j = peer(d)
        wait_from(2, all_strain, j)
        answer = answer + meet(j)
    total = answer[:, :width]
    for k in range(1, per_tile):
        total = total + answer[:, k * width : (k + 1) * width]
    out_ref[...] = total[0]
    for copy in copies:
        copy.wait_send()


def square_kernel(
    events_hbm, counts_hbm, resid_hbm, green_hbm, strain_hbm, out_ref,
    events_ref, counts_ref, resid, green, strain,
    send_head, own_head, far_head, send_field, own_field, far_field,
    send_tail, own_tail, far_tail, send_bits, own_bits, far_bits, own_wide, far_wide,
    waves, rows_of, toeplitz, head_sum, tail_sum, side_sum, load_sem, send_sem, recv_sem,
):
    me = lax.axis_index("sta")
    x, y = lax.rem(me, 2), me // 2
    odd = lax.rem(x + y, 2)
    beside = me + 1 - 2 * x
    above = lax.rem(me + 2, 4)
    first = beside + odd * (above - beside)
    second = above + odd * (beside - above)
    across = 3 - me
    comps, nt, vox = green.shape
    local_events = strain.shape[0]
    events = waves.shape[1]
    width = vox // 4
    per_tile = LANES // width
    rest = comps - per_tile
    half = nt // 2

    barrier = pltpu.get_barrier_semaphore()
    for target in (first, second):
        pl.semaphore_signal(
            barrier, inc=1, device_id={"sta": target}, device_id_type=pl.DeviceIdType.MESH
        )

    loads = {}
    for name, src, dst in (
        ("green", green_hbm.at[0], green),
        ("events", events_hbm, events_ref),
        ("counts", counts_hbm, counts_ref),
        ("resid", resid_hbm, resid),
        ("strain", strain_hbm, strain),
    ):
        loads[name] = pltpu.make_async_copy(src, dst, load_sem.at[len(loads)])
        loads[name].start()

    low_half, high_half = pl.ds(0, LANES), pl.ds(LANES, LANES)
    plan = {}
    for name, src, dst, target in (
        ("u0h", send_head.at[0], far_head.at[2], first),
        ("u2h", far_head.at[0], own_head.at[2], first),
        ("u3h", far_head.at[2], own_head.at[3], first),
        ("w1h", send_head.at[1], own_head.at[1], second),
        ("w0h", own_head.at[0], far_head.at[1], second),
        ("w4h", own_head.at[1], far_head.at[3], second),
        ("u0t", send_tail.at[0], far_tail.at[2], first),
        ("u2t", far_tail.at[0], own_tail.at[2], first),
        ("u3t", far_tail.at[2], own_tail.at[3], first),
        ("w1t", send_tail.at[1], own_tail.at[1], second),
        ("w0t", own_tail.at[0], far_tail.at[1], second),
        ("w4t", own_tail.at[1], far_tail.at[3], second),
        ("wave1", waves.at[0], waves.at[2], first),
        ("wave2", waves.at[0], waves.at[1], second),
        ("wave3", waves.at[2, :, low_half], waves.at[3, :, low_half], first),
        ("wave4", waves.at[1, :, high_half], waves.at[3, :, high_half], second),
        ("side", side_sum.at[0], side_sum.at[1], first),
        *(
            item
            for e in range(local_events)
            for item in (
                (f"u1h{e}", send_field.at[0, e], far_field.at[1, e], first),
                (f"w2h{e}", send_field.at[1, e], own_field.at[1, e], second),
                (f"u1t{e}", send_bits.at[0, e], far_bits.at[1, e], first),
                (f"w2t{e}", send_bits.at[1, e], own_bits.at[1, e], second),
            )
        ),
    ):
        plan[name] = pltpu.make_async_remote_copy(
            src_ref=src,
            dst_ref=dst,
            send_sem=send_sem.at[len(plan)],
            recv_sem=recv_sem.at[len(plan)],
            device_id={"sta": target},
            device_id_type=pl.DeviceIdType.MESH,
        )

    def start(*names):
        for name in names:
            plan[name].start()

    def arrive(*names):
        for name in names:
            plan[name].wait_recv()

    each = range(local_events)
    lane = lax.broadcasted_iota(jnp.int32, (LANES, LANES), 0)
    column = lax.broadcasted_iota(jnp.int32, (LANES, LANES), 1)
    later = column >= lane
    low = column < LANES // 2

    def picker(j):
        parts = []
        for slot in range(per_tile):
            inside = (column >= slot * width) & (column < (slot + 1) * width)
            hit = inside & (lane == column + (j - slot) * width)
            parts.append(jnp.where(hit, 1.0, 0.0).astype(BF16))
        return jnp.concatenate(parts, axis=0)

    def packed(pieces, matrix):
        wide = jnp.concatenate(pieces, axis=1)
        return jnp.dot(wide, matrix, preferred_element_type=F32).astype(BF16)

    def head_of(source, matrix):
        return packed([source[k] for k in range(per_tile)], matrix)

    def tail_of(source, matrix):
        return packed(
            [source[per_tile + k, h * half : (h + 1) * half] for h in range(2) for k in range(rest)],
            matrix,
        )

    def make_toeplitz(s):
        rows_of[...] = waves[s].astype(F32)

        @pl.loop(0, 3 * local_events)
        def _(k):
            group = k // local_events
            owner = me + (group % 2) * (first - me) + (group // 2) * (second - me)
            wave = rows_of[pl.ds(owner * local_events + k - group * local_events, 1), :]
            before = 0.0
            for b in range(2):
                piece = jnp.broadcast_to(wave[:, b * LANES : (b + 1) * LANES], (LANES, LANES))
                turned = pltpu.roll(piece, 0, 1, stride=1, stride_axis=0)
                toeplitz[k, s, b] = jnp.where(later, turned, before).astype(BF16)
                before = turned

    def widen(source, s, dst):
        piece = source[s].astype(F32)
        dst[s, :half] = source[s]
        dst[s, half:] = jnp.where(low, pltpu.roll(piece, LANES // 2, 1), 0.0).astype(BF16)

    nothing = jnp.zeros((half, half), BF16)

    def head_dot(k, stations, heads):
        top = [toeplitz[k, s, b] for s in stations for b in range(2)]
        bottom = [piece for s in stations for piece in (nothing, toeplitz[k, s, 0])]
        matrix = jnp.concatenate(
            [jnp.concatenate(top, axis=1), jnp.concatenate(bottom, axis=1)], axis=0
        )
        stack = jnp.concatenate([heads[s] for s in stations], axis=0)
        return jnp.dot(matrix, stack, preferred_element_type=F32)

    def tail_dot(k, stations, wides):
        matrix = jnp.concatenate([toeplitz[k, s, b] for s in stations for b in range(2)], axis=1)
        stack = jnp.concatenate([wides[s] for s in stations], axis=0)
        return jnp.dot(matrix, stack, preferred_element_type=F32)

    def met(field, adjoint):
        return jnp.sum(field.astype(F32) * adjoint, axis=0, keepdims=True)

    to_across, to_second = picker(across), picker(second)
    loads["green"].wait()
    send_head[0] = head_of(green, to_across)
    pl.semaphore_wait(barrier, 2)
    start("u0h")
    send_head[1] = head_of(green, to_second)
    start("w1h")

    for name in ("events", "counts", "resid"):
        loads[name].wait()
    rows = lax.broadcasted_iota(jnp.int32, (events, nt), 0)
    comb = jnp.zeros((events, nt), F32)
    for p in range(resid.shape[1]):
        event = jnp.where(p < counts_ref[0], events_ref[0, p], -1)
        comb = comb + jnp.where(rows == event, resid[0, p : p + 1, :], 0.0)
    waves[0] = comb.astype(BF16)
    start("wave1", "wave2")

    send_tail[0] = tail_of(green, to_across)
    send_tail[1] = tail_of(green, to_second)
    start("u0t", "w1t")
    to_me, to_first = picker(me), picker(first)
    own_head[0] = head_of(green, to_me)
    loads["strain"].wait()
    send_field[0, 0] = head_of(strain.at[0], to_across)
    start("w0h", "u1h0")
    arrive("wave1", "wave2")
    start("wave3", "wave4")
    for e in each[1:]:
        send_field[0, e] = head_of(strain.at[e], to_across)
        start(f"u1h{e}")
    own_tail[0] = tail_of(green, to_me)
    for e in each:
        send_bits[0, e] = tail_of(strain.at[e], to_across)
    arrive("w1h")
    start("w4h", "w0t")
    for e in each:
        start(f"u1t{e}")
    arrive("w1t")
    start("w4t")
    far_head[0] = head_of(green, to_first)
    start("u2h")
    for e in each:
        send_field[1, e] = head_of(strain.at[e], to_second)
        start(f"w2h{e}")
    arrive("u0h")
    start("u3h")
    far_tail[0] = tail_of(green, to_first)
    for e in each:
        send_bits[1, e] = tail_of(strain.at[e], to_second)
        start(f"w2t{e}")
    make_toeplitz(0)
    make_toeplitz(1)
    make_toeplitz(2)
    for e in each:
        far_field[0, e] = head_of(strain.at[e], to_first)
        far_bits[0, e] = tail_of(strain.at[e], to_first)
        own_field[0, e] = head_of(strain.at[e], to_me)
        own_bits[0, e] = tail_of(strain.at[e], to_me)
    widen(own_tail, 0, own_wide)
    widen(own_tail, 1, own_wide)
    widen(far_tail, 0, far_wide)
    arrive("u0t")
    widen(far_tail, 2, far_wide)
    arrive("wave3", "wave4")
    start("u2t", "u3t")
    make_toeplitz(3)

    arrive("w0h", "w4h")
    for e in each:
        arrive(f"u1h{e}")
    part = jnp.zeros((1, LANES), F32)
    for side, base in ((0, 0), (1, 2 * local_events)):
        for e in each:
            part = part + met(far_field[side, e], head_dot(base + e, range(4), far_head))
    arrive("w0t", "w4t")
    widen(far_tail, 1, far_wide)
    widen(far_tail, 3, far_wide)
    for e in each:
        arrive(f"u1t{e}")
    for side, base in ((0, 0), (1, 2 * local_events)):
        for e in each:
            part = part + met(far_bits[side, e], tail_dot(base + e, range(4), far_wide))
    side_sum[0] = part
    start("side")

    for k in range(2 * local_events):
        head_sum[k] = head_dot(k, range(2), own_head)
    arrive("u2h")
    for k in range(2 * local_events):
        head_sum[k] += head_dot(k, (2,), own_head)
    arrive("u3h")
    for e in each:
        arrive(f"w2h{e}")
    part = jnp.zeros((1, LANES), F32)
    for g in range(2):
        for e in each:
            k = g * local_events + e
            part = part + met(own_field[g, e], head_sum[k] + head_dot(k, (3,), own_head))
    arrive("u2t")
    widen(own_tail, 2, own_wide)
    for k in range(2 * local_events):
        tail_sum[k] = tail_dot(k, range(3), own_wide)
    arrive("u3t")
    widen(own_tail, 3, own_wide)
    for e in each:
        arrive(f"w2t{e}")
    for g in range(2):
        for e in each:
            k = g * local_events + e
            part = part + met(own_bits[g, e], tail_sum[k] + tail_dot(k, (3,), own_wide))
    arrive("side")
    answer = part + side_sum[1]
    total = answer[:, :width]
    for k in range(1, per_tile):
        total = total + answer[:, k * width : (k + 1) * width]
    out_ref[...] = total[0]
    for copy in plan.values():
        copy.wait_send()


def solution(mesh):
    n = mesh.shape["sta"]

    def body(green_tensor, strain, pair_events, pair_counts, residuals):
        _, comps, nt, vox = green_tensor.shape
        local_events = strain.shape[0]
        width = vox // n
        per_tile = LANES // width
        full = comps // per_tile
        rest = comps % per_tile
        fit = min(per_tile // rest, local_events) if rest else 1
        green_tiles = full + (1 if rest else 0)
        strain_tiles = full * local_events + (local_events // fit if rest else 0)
        events = n * local_events
        square = n == 4 and nt == 2 * LANES and full == 1 and 2 * rest == per_tile
        if square:
            steps = square_kernel
            pairs = pair_events.shape[1]
            half = nt // 2
            copies = 17 + 4 * local_events
            scratch = [
                pltpu.SMEM((1, pairs), jnp.int32),
                pltpu.SMEM((1,), jnp.int32),
                pltpu.VMEM((1, pairs, nt), F32),
                pltpu.VMEM((comps, nt, vox), BF16),
                pltpu.VMEM((local_events, comps, nt, vox), BF16),
                *(pltpu.VMEM((k, nt, LANES), BF16) for k in (2, 4, 4)),
                *(pltpu.VMEM((2, local_events, nt, LANES), BF16) for _ in range(3)),
                *(pltpu.VMEM((k, half, LANES), BF16) for k in (2, 4, 4)),
                *(pltpu.VMEM((2, local_events, half, LANES), BF16) for _ in range(3)),
                *(pltpu.VMEM((4, nt, LANES), BF16) for _ in range(2)),
                pltpu.VMEM((4, events, nt), BF16),
                pltpu.VMEM((events, nt), F32),
                pltpu.VMEM((3 * local_events, 4, 2, half, half), BF16),
                pltpu.VMEM((2 * local_events, nt, LANES), F32),
                pltpu.VMEM((2 * local_events, half, LANES), F32),
                pltpu.VMEM((2, 1, LANES), F32),
                pltpu.SemaphoreType.DMA((5,)),
                pltpu.SemaphoreType.DMA((copies,)),
                pltpu.SemaphoreType.DMA((copies,)),
            ]
        else:
            steps = functools.partial(kernel, n)
            scratch = [
                pltpu.VMEM((comps, nt, vox), BF16),
                pltpu.VMEM((local_events, comps, nt, vox), BF16),
                pltpu.VMEM((n, green_tiles, nt, LANES), BF16),
                pltpu.VMEM((n, strain_tiles, nt, LANES), BF16),
                pltpu.VMEM((n, events, nt), F32),
                pltpu.VMEM((n, green_tiles, nt, LANES), BF16),
                pltpu.VMEM((n, strain_tiles, nt, LANES), BF16),
                pltpu.VMEM((events, nt, green_tiles * LANES), F32),
                pltpu.SemaphoreType.DMA((2,)),
                pltpu.SemaphoreType.DMA((3, n)),
                pltpu.SemaphoreType.DMA((3, n)),
            ]
        if square:
            return pl.pallas_call(
                steps,
                out_shape=pltpu.VMEM((width,), F32),
                in_specs=[pl.BlockSpec(memory_space=pl.ANY)] * 5,
                out_specs=pl.BlockSpec(memory_space=pltpu.VMEM),
                scratch_shapes=scratch,
                compiler_params=pltpu.CompilerParams(collective_id=0, has_side_effects=True),
            )(pair_events, pair_counts, residuals, green_tensor, strain)
        return pl.pallas_call(
            steps,
            out_shape=jax.ShapeDtypeStruct((width,), F32),
            in_specs=[
                pl.BlockSpec(memory_space=pltpu.SMEM),
                pl.BlockSpec(memory_space=pltpu.SMEM),
                pl.BlockSpec(memory_space=pltpu.VMEM),
                pl.BlockSpec(memory_space=pl.ANY),
                pl.BlockSpec(memory_space=pl.ANY),
            ],
            out_specs=pl.BlockSpec(memory_space=pltpu.VMEM),
            scratch_shapes=scratch,
            compiler_params=pltpu.CompilerParams(collective_id=0, has_side_effects=True),
        )(pair_events, pair_counts, residuals[0], green_tensor, strain)

    in_specs = (
        P("sta", None, None, "vox"),
        P("sta", None, None, "vox"),
        P("sta", None),
        P("sta"),
        P("sta", None, None),
    )
    out_specs = P(("vox", "sta"))
    return jax.shard_map(body, mesh=mesh, in_specs=in_specs, out_specs=out_specs, check_vma=False)
```

```python
import functools

import jax
import jax.numpy as jnp
from jax import lax
from jax.experimental import pallas as pl
from jax.experimental.pallas import tpu as pltpu
from jax.sharding import PartitionSpec as P

LANES = 128
F32 = jnp.float32
BF16 = jnp.bfloat16


def kernel(
    n, events_ref, counts_ref, resid_ref, green_hbm, strain_hbm, out_ref,
    green, strain, packed_green, packed_strain, all_comb, all_green, all_strain, adjoint,
    load_sem, send_sem, recv_sem,
):
    me = lax.axis_index("sta")
    comps, nt, vox = green.shape
    local_events = strain.shape[0]
    slots = resid_ref.shape[0]
    width = vox // n
    per_tile = LANES // width
    full = comps // per_tile
    rest = comps % per_tile
    fit = min(per_tile // rest, local_events) if rest else 1
    blocks = nt // LANES

    def peer(d):
        pair = lax.rem(me // 2 + d // 2, n // 2)
        return 2 * pair + lax.rem(me + d, 2)

    order = list(range(n - 1, 0, -1))
    load_green = pltpu.make_async_copy(green_hbm.at[0], green, load_sem.at[0])
    load_strain = pltpu.make_async_copy(strain_hbm, strain, load_sem.at[1])
    load_green.start()
    load_strain.start()

    barrier = pltpu.get_barrier_semaphore()
    for d in order:
        pl.semaphore_signal(
            barrier, inc=1, device_id={"sta": peer(d)}, device_id_type=pl.DeviceIdType.MESH
        )

    def send(kind, src, dst, d):
        copy = pltpu.make_async_remote_copy(
            src_ref=src,
            dst_ref=dst.at[me],
            send_sem=send_sem.at[kind, d],
            recv_sem=recv_sem.at[kind, me],
            device_id={"sta": peer(d)},
            device_id_type=pl.DeviceIdType.MESH,
        )
        copy.start()
        return copy

    def wait_from(kind, dst, j):
        pltpu.make_async_remote_copy(
            src_ref=dst.at[j],
            dst_ref=dst.at[j],
            send_sem=send_sem.at[kind, 0],
            recv_sem=recv_sem.at[kind, j],
            device_id={"sta": j},
            device_id_type=pl.DeviceIdType.MESH,
        ).wait_recv()

    rows = lax.broadcasted_iota(jnp.int32, (all_comb.shape[1], nt), 0)
    comb = jnp.zeros((all_comb.shape[1], nt), F32)
    for p in range(slots):
        event = jnp.where(p < counts_ref[0], events_ref[0, p], -1)
        comb = comb + jnp.where(rows == event, resid_ref[p : p + 1, :], 0.0)
    all_comb[me] = comb

    lane = lax.broadcasted_iota(jnp.int32, (LANES, LANES), 0)
    column = lax.broadcasted_iota(jnp.int32, (LANES, LANES), 1)

    def pick(j, slot):
        inside = (column >= slot * width) & (column < (slot + 1) * width)
        return inside & (lane == column + (j - slot) * width)

    def as_matrix(masks):
        return jnp.concatenate([jnp.where(m, 1.0, 0.0).astype(BF16) for m in masks], axis=0)

    def gathered(tiles, matrix):
        wide = jnp.concatenate(tiles, axis=1)
        return jnp.dot(wide, matrix[: len(tiles) * LANES], preferred_element_type=F32).astype(BF16)

    def pack_green(j, masks, matrix, dst, index):
        for a in range(full):
            dst[index, a] = gathered([green[a * per_tile + k] for k in range(per_tile)], matrix)
        if rest:
            repeated = []
            for k in range(rest):
                hit = masks[k]
                for i in range(1, fit):
                    hit = hit | masks[i * rest + k]
                repeated.append(hit)
            dst[index, full] = gathered(
                [green[full * per_tile + k] for k in range(rest)], as_matrix(repeated)
            )

    def pack_strain(matrix, dst, index):
        tile = 0
        for e in range(local_events):
            for a in range(full):
                dst[index, tile] = gathered(
                    [strain[e, a * per_tile + k] for k in range(per_tile)], matrix
                )
                tile += 1
        if rest:
            for e in range(0, local_events, fit):
                dst[index, tile] = gathered(
                    [strain[e + i, full * per_tile + k] for i in range(fit) for k in range(rest)],
                    matrix,
                )
                tile += 1

    matrices = {}
    for d in order + [0]:
        j = peer(d)
        masks = [pick(j, slot) for slot in range(per_tile)]
        matrices[d] = (j, masks, as_matrix(masks))

    load_green.wait()
    copies = []
    pl.semaphore_wait(barrier, n - 1)
    for d in order:
        copies.append(send(0, all_comb.at[me], all_comb, d))
    waiting = None
    for d in order:
        pack_green(*matrices[d], packed_green, d)
        if waiting is not None:
            copies.append(send(1, packed_green.at[waiting], all_green, waiting))
        waiting = d
    pack_green(*matrices[0], all_green, me)
    copies.append(send(1, packed_green.at[waiting], all_green, waiting))
    load_strain.wait()
    waiting = None
    for d in order:
        pack_strain(matrices[d][2], packed_strain, d)
        if waiting is not None:
            copies.append(send(2, packed_strain.at[waiting], all_strain, waiting))
        waiting = d
    pack_strain(matrices[0][2], all_strain, me)
    copies.append(send(2, packed_strain.at[waiting], all_strain, waiting))

    for d in order:
        wait_from(0, all_comb, peer(d))
    for d in order:
        wait_from(1, all_green, peer(d))

    later = column >= lane
    nothing = jnp.zeros((LANES, LANES), BF16)
    tiles = all_green.shape[1]

    @pl.loop(0, all_comb.shape[1])
    def _(e):
        total = jnp.zeros((nt, tiles * LANES), F32)
        for s in range(n):
            wave = all_comb[s, pl.ds(e, 1), :]
            turned = []
            for k in range(blocks):
                piece = jnp.broadcast_to(wave[:, k * LANES : (k + 1) * LANES], (LANES, LANES))
                turned.append(pltpu.roll(piece, 0, 1, stride=1, stride_axis=0))
            diag = [
                jnp.where(later, turned[k], turned[k - 1] if k else 0.0).astype(BF16)
                for k in range(blocks)
            ]
            matrix = jnp.concatenate(
                [
                    jnp.concatenate([nothing] * i + diag[: blocks - i], axis=1)
                    for i in range(blocks)
                ],
                axis=0,
            )
            field = jnp.concatenate([all_green[s, t] for t in range(tiles)], axis=1)
            total = total + jnp.dot(matrix, field, preferred_element_type=F32)
        adjoint[e] = total

    spot = lax.broadcasted_iota(jnp.int32, (nt, LANES), 1)

    def meet(j):
        part = jnp.zeros((1, LANES), F32)
        tile = 0
        for e in range(local_events):
            for a in range(full):
                field = all_strain[j, tile].astype(F32)
                one = adjoint[j * local_events + e, :, a * LANES : (a + 1) * LANES]
                part = part + jnp.sum(field * one, axis=0, keepdims=True)
                tile += 1
        if rest:
            for e in range(0, local_events, fit):
                field = all_strain[j, tile].astype(F32)
                one = adjoint[j * local_events + e, :, full * LANES :]
                for i in range(1, fit):
                    other = adjoint[j * local_events + e + i, :, full * LANES :]
                    one = jnp.where(spot < i * rest * width, one, other)
                part = part + jnp.sum(
                    jnp.where(spot < fit * rest * width, field * one, 0.0), axis=0, keepdims=True
                )
                tile += 1
        return part

    answer = meet(me)
    for d in order:
        j = peer(d)
        wait_from(2, all_strain, j)
        answer = answer + meet(j)
    total = answer[:, :width]
    for k in range(1, per_tile):
        total = total + answer[:, k * width : (k + 1) * width]
    out_ref[...] = total[0]
    for copy in copies:
        copy.wait_send()


def square_kernel(
    events_hbm, counts_hbm, resid_hbm, green_hbm, strain_hbm, out_ref,
    events_ref, counts_ref, resid, green, strain,
    send_head, own_head, far_head, send_field, own_field, far_field,
    send_tail, own_tail, far_tail, send_bits, own_bits, far_bits, own_wide, far_wide,
    waves, rows_of, toeplitz, head_sum, tail_sum, far_head_sum, far_tail_sum, side_sum, load_sem, send_sem, recv_sem,
):
    me = lax.axis_index("sta")
    x, y = lax.rem(me, 2), me // 2
    odd = lax.rem(x + y, 2)
    beside = me + 1 - 2 * x
    above = lax.rem(me + 2, 4)
    first = beside + odd * (above - beside)
    second = above + odd * (beside - above)
    across = 3 - me
    comps, nt, vox = green.shape
    local_events = strain.shape[0]
    events = waves.shape[1]
    width = vox // 4
    per_tile = LANES // width
    rest = comps - per_tile
    half = nt // 2

    barrier = pltpu.get_barrier_semaphore()
    for target in (first, second):
        pl.semaphore_signal(
            barrier, inc=1, device_id={"sta": target}, device_id_type=pl.DeviceIdType.MESH
        )

    loads = {}
    for name, src, dst in (
        ("green", green_hbm.at[0], green),
        ("events", events_hbm, events_ref),
        ("counts", counts_hbm, counts_ref),
        ("resid", resid_hbm, resid),
        ("strain", strain_hbm, strain),
    ):
        loads[name] = pltpu.make_async_copy(src, dst, load_sem.at[len(loads)])
        loads[name].start()

    low_half, high_half = pl.ds(0, LANES), pl.ds(LANES, LANES)
    plan = {}
    for name, src, dst, target in (
        ("u0h", send_head.at[0], far_head.at[2], first),
        ("u2h", far_head.at[0], own_head.at[2], first),
        ("u3h", far_head.at[2], own_head.at[3], first),
        ("w1h", send_head.at[1], own_head.at[1], second),
        ("w0h", own_head.at[0], far_head.at[1], second),
        ("w4h", own_head.at[1], far_head.at[3], second),
        ("u0t", send_tail.at[0], far_tail.at[2], first),
        ("u2t", far_tail.at[0], own_tail.at[2], first),
        ("u3t", far_tail.at[2], own_tail.at[3], first),
        ("w1t", send_tail.at[1], own_tail.at[1], second),
        ("w0t", own_tail.at[0], far_tail.at[1], second),
        ("w4t", own_tail.at[1], far_tail.at[3], second),
        ("wave1", waves.at[0], waves.at[2], first),
        ("wave2", waves.at[0], waves.at[1], second),
        ("wave3", waves.at[2, :, low_half], waves.at[3, :, low_half], first),
        ("wave4", waves.at[1, :, high_half], waves.at[3, :, high_half], second),
        ("side", side_sum.at[0], side_sum.at[1], first),
        *(
            item
            for e in range(local_events)
            for item in (
                (f"u1h{e}", send_field.at[0, e], far_field.at[1, e], first),
                (f"w2h{e}", send_field.at[1, e], own_field.at[1, e], second),
                (f"u1t{e}", send_bits.at[0, e], far_bits.at[1, e], first),
                (f"w2t{e}", send_bits.at[1, e], own_bits.at[1, e], second),
            )
        ),
    ):
        plan[name] = pltpu.make_async_remote_copy(
            src_ref=src,
            dst_ref=dst,
            send_sem=send_sem.at[len(plan)],
            recv_sem=recv_sem.at[len(plan)],
            device_id={"sta": target},
            device_id_type=pl.DeviceIdType.MESH,
        )

    core = lax.rem(lax.axis_index("vox"), 2)

    def start(*names):
        for name in names:
            plan[name].start()

    def start_on(which, *names):
        @pl.when(core == which)
        def _():
            start(*names)

    def arrive(*names):
        for name in names:
            plan[name].wait_recv()

    each = range(local_events)
    lane = lax.broadcasted_iota(jnp.int32, (LANES, LANES), 0)
    column = lax.broadcasted_iota(jnp.int32, (LANES, LANES), 1)
    later = column >= lane
    low = column < LANES // 2

    def picker(j):
        parts = []
        for slot in range(per_tile):
            inside = (column >= slot * width) & (column < (slot + 1) * width)
            hit = inside & (lane == column + (j - slot) * width)
            parts.append(jnp.where(hit, 1.0, 0.0).astype(BF16))
        return jnp.concatenate(parts, axis=0)

    def wide_head(source):
        return jnp.concatenate([source[k] for k in range(per_tile)], axis=1)

    def wide_tail(source):
        return jnp.concatenate(
            [source[per_tile + k, h * half : (h + 1) * half] for h in range(2) for k in range(rest)],
            axis=1,
        )

    def pack(wides, pickers, *outs):
        wide = jnp.concatenate(wides, axis=0)
        both = jnp.dot(wide, pickers, preferred_element_type=F32).astype(BF16)
        at = 0
        for left, right in outs:
            size = left.shape[0]
            left[...] = both[at : at + size, :LANES]
            right[...] = both[at : at + size, LANES:]
            at += size

    def make_toeplitz(s):
        rows_of[...] = waves[s].astype(F32)

        for k in range(3 * local_events):
            owner = (me, first, second)[k // local_events]
            wave = rows_of[pl.ds(owner * local_events + k % local_events, 1), :]
            before = 0.0
            for b in range(2):
                piece = jnp.broadcast_to(wave[:, b * LANES : (b + 1) * LANES], (LANES, LANES))
                turned = pltpu.roll(piece, 0, 1, stride=1, stride_axis=0)
                toeplitz[k, s, b] = jnp.where(later, turned, before).astype(BF16)
                before = turned

    def widen(source, s, dst):
        piece = source[s].astype(F32)
        dst[s, :half] = source[s]
        dst[s, half:] = jnp.where(low, pltpu.roll(piece, LANES // 2, 1), 0.0).astype(BF16)

    nothing = jnp.zeros((half, half), BF16)

    def top(k, stations):
        return jnp.concatenate([toeplitz[k, s, b] for s in stations for b in range(2)], axis=1)

    def bottom(k, stations):
        return jnp.concatenate(
            [piece for s in stations for piece in (nothing, toeplitz[k, s, 0])], axis=1
        )

    def stack(fields, stations):
        return jnp.concatenate([fields[s] for s in stations], axis=0)

    def head_dot(ks, stations, field):
        matrix = jnp.concatenate([f(k, stations) for k in ks for f in (top, bottom)], axis=0)
        return jnp.dot(matrix, field, preferred_element_type=F32)

    def tail_dot(ks, stations, field):
        matrix = jnp.concatenate([top(k, stations) for k in ks], axis=0)
        return jnp.dot(matrix, field, preferred_element_type=F32)

    def met(field, adjoint):
        return jnp.sum(field.astype(F32) * adjoint, axis=0, keepdims=True)

    away = jnp.concatenate([picker(across), picker(second)], axis=1)
    loads["green"].wait()
    pack([wide_head(green)], away, (send_head.at[0], send_head.at[1]))
    pl.semaphore_wait(barrier, 2)
    start("u0h", "w1h")

    for name in ("events", "counts", "resid"):
        loads[name].wait()
    rows = lax.broadcasted_iota(jnp.int32, (events, nt), 0)
    comb = jnp.zeros((events, nt), F32)
    for p in range(resid.shape[1]):
        event = jnp.where(p < counts_ref[0], events_ref[0, p], -1)
        comb = comb + jnp.where(rows == event, resid[0, p : p + 1, :], 0.0)
    waves[0] = comb.astype(BF16)
    start("wave1", "wave2")

    pack([wide_tail(green)], away, (send_tail.at[0], send_tail.at[1]))
    start("u0t", "w1t")
    near = jnp.concatenate([picker(me), picker(first)], axis=1)
    pack(
        [wide_head(green), wide_tail(green)],
        near,
        (own_head.at[0], far_head.at[0]),
        (own_tail.at[0], far_tail.at[0]),
    )
    start("w0h", "w0t")
    loads["strain"].wait()
    pack(
        [f(strain.at[e]) for f in (wide_head, wide_tail) for e in each],
        away,
        *((send_field.at[0, e], send_field.at[1, e]) for e in each),
        *((send_bits.at[0, e], send_bits.at[1, e]) for e in each),
    )
    start("u1h0", "u1h1")
    arrive("wave1", "wave2")
    start("wave3", "wave4", "u1t0", "u1t1")
    arrive("w1h")
    start("w4h")
    arrive("w1t")
    start("w4t")
    start_on(0, "u2h", "w2h0", "w2h1")
    arrive("u0h")
    start_on(0, "u3h", "u2t", "w2t0", "w2t1")
    arrive("u0t")
    start_on(0, "u3t")
    pack(
        [f(strain.at[e]) for f in (wide_head, wide_tail) for e in each],
        near,
        *((own_field.at[0, e], far_field.at[0, e]) for e in each),
        *((own_bits.at[0, e], far_bits.at[0, e]) for e in each),
    )
    early, late = range(2), (3,)
    ours = range(2 * local_events)
    theirs = [*each, *range(2 * local_events, 3 * local_events)]

    def gather(ks, stations, heads, wides, heads_to, tails_to, fresh):
        field = jnp.concatenate([stack(heads, stations), stack(wides, stations)], axis=1)
        both = head_dot(ks, stations, field)
        for i in ours:
            head, tail = both[i * nt : (i + 1) * nt, :LANES], both[i * nt : i * nt + half, LANES:]
            heads_to[i] = head if fresh else heads_to[i] + head
            tails_to[i] = tail if fresh else tails_to[i] + tail

    make_toeplitz(0)
    make_toeplitz(2)
    widen(far_tail, 0, far_wide)
    widen(far_tail, 2, far_wide)
    gather(theirs, (0, 2), far_head, far_wide, far_head_sum, far_tail_sum, True)
    make_toeplitz(1)
    widen(own_tail, 0, own_wide)
    widen(own_tail, 1, own_wide)
    gather(ours, early, own_head, own_wide, head_sum, tail_sum, True)
    arrive("wave3", "wave4")
    make_toeplitz(3)
    arrive("w0h", "w0t")
    start_on(1, "w2h0", "u2h")
    widen(far_tail, 1, far_wide)
    gather(theirs, (1,), far_head, far_wide, far_head_sum, far_tail_sum, False)
    arrive("w4h", "w4t")
    start_on(1, "w2h1", "u3h", "u2t", "w2t0", "w2t1", "u3t")
    widen(far_tail, 3, far_wide)
    field = jnp.concatenate([far_head[3], far_wide[3]], axis=1)
    both = head_dot(theirs, late, field)
    for e in each:
        arrive(f"u1h{e}", f"u1t{e}")
    part = jnp.zeros((1, LANES), F32)
    for i in ours:
        side, e = i // local_events, i % local_events
        head, tail = both[i * nt : (i + 1) * nt, :LANES], both[i * nt : i * nt + half, LANES:]
        part = part + met(far_field[side, e], far_head_sum[i] + head)
        part = part + met(far_bits[side, e], far_tail_sum[i] + tail)
    side_sum[0] = part
    start("side")

    arrive("u2h")
    two = head_dot(ours, (2,), own_head[2])
    for k in ours:
        head_sum[k] += two[k * nt : (k + 1) * nt]
    arrive("u3h")
    three = head_dot(ours, late, own_head[3])
    for e in each:
        arrive(f"w2h{e}")
    part = jnp.zeros((1, LANES), F32)
    for k in ours:
        field = own_field[k // local_events, k % local_events]
        part = part + met(field, head_sum[k] + three[k * nt : (k + 1) * nt])
    arrive("u2t")
    widen(own_tail, 2, own_wide)
    two = tail_dot(ours, (2,), own_wide[2])
    for k in ours:
        tail_sum[k] += two[k * half : (k + 1) * half]
    arrive("u3t")
    widen(own_tail, 3, own_wide)
    three = tail_dot(ours, late, own_wide[3])
    for e in each:
        arrive(f"w2t{e}")
    for k in ours:
        field = own_bits[k // local_events, k % local_events]
        part = part + met(field, tail_sum[k] + three[k * half : (k + 1) * half])
    arrive("side")
    answer = part + side_sum[1]
    total = answer[:, :width]
    for k in range(1, per_tile):
        total = total + answer[:, k * width : (k + 1) * width]
    out_ref[...] = total[0]
    for copy in plan.values():
        copy.wait_send()


def solution(mesh):
    n = mesh.shape["sta"]

    def body(green_tensor, strain, pair_events, pair_counts, residuals):
        _, comps, nt, vox = green_tensor.shape
        local_events = strain.shape[0]
        width = vox // n
        per_tile = LANES // width
        full = comps // per_tile
        rest = comps % per_tile
        fit = min(per_tile // rest, local_events) if rest else 1
        green_tiles = full + (1 if rest else 0)
        strain_tiles = full * local_events + (local_events // fit if rest else 0)
        events = n * local_events
        square = n == 4 and nt == 2 * LANES and full == 1 and 2 * rest == per_tile
        if square:
            steps = square_kernel
            pairs = pair_events.shape[1]
            half = nt // 2
            copies = 17 + 4 * local_events
            scratch = [
                pltpu.SMEM((1, pairs), jnp.int32),
                pltpu.SMEM((1,), jnp.int32),
                pltpu.VMEM((1, pairs, nt), F32),
                pltpu.VMEM((comps, nt, vox), BF16),
                pltpu.VMEM((local_events, comps, nt, vox), BF16),
                *(pltpu.VMEM((k, nt, LANES), BF16) for k in (2, 4, 4)),
                *(pltpu.VMEM((2, local_events, nt, LANES), BF16) for _ in range(3)),
                *(pltpu.VMEM((k, half, LANES), BF16) for k in (2, 4, 4)),
                *(pltpu.VMEM((2, local_events, half, LANES), BF16) for _ in range(3)),
                *(pltpu.VMEM((4, nt, LANES), BF16) for _ in range(2)),
                pltpu.VMEM((4, events, nt), BF16),
                pltpu.VMEM((events, nt), F32),
                pltpu.VMEM((3 * local_events, 4, 2, half, half), BF16),
                pltpu.VMEM((2 * local_events, nt, LANES), F32),
                pltpu.VMEM((2 * local_events, half, LANES), F32),
                pltpu.VMEM((2 * local_events, nt, LANES), F32),
                pltpu.VMEM((2 * local_events, half, LANES), F32),
                pltpu.VMEM((2, 1, LANES), F32),
                pltpu.SemaphoreType.DMA((5,)),
                pltpu.SemaphoreType.DMA((copies,)),
                pltpu.SemaphoreType.DMA((copies,)),
            ]
        else:
            steps = functools.partial(kernel, n)
            scratch = [
                pltpu.VMEM((comps, nt, vox), BF16),
                pltpu.VMEM((local_events, comps, nt, vox), BF16),
                pltpu.VMEM((n, green_tiles, nt, LANES), BF16),
                pltpu.VMEM((n, strain_tiles, nt, LANES), BF16),
                pltpu.VMEM((n, events, nt), F32),
                pltpu.VMEM((n, green_tiles, nt, LANES), BF16),
                pltpu.VMEM((n, strain_tiles, nt, LANES), BF16),
                pltpu.VMEM((events, nt, green_tiles * LANES), F32),
                pltpu.SemaphoreType.DMA((2,)),
                pltpu.SemaphoreType.DMA((3, n)),
                pltpu.SemaphoreType.DMA((3, n)),
            ]
        if square:
            return pl.pallas_call(
                steps,
                out_shape=pltpu.VMEM((width,), F32),
                in_specs=[pl.BlockSpec(memory_space=pl.ANY)] * 5,
                out_specs=pl.BlockSpec(memory_space=pltpu.VMEM),
                scratch_shapes=scratch,
                compiler_params=pltpu.CompilerParams(collective_id=0, has_side_effects=True),
            )(pair_events, pair_counts, residuals, green_tensor, strain)
        return pl.pallas_call(
            steps,
            out_shape=jax.ShapeDtypeStruct((width,), F32),
            in_specs=[
                pl.BlockSpec(memory_space=pltpu.SMEM),
                pl.BlockSpec(memory_space=pltpu.SMEM),
                pl.BlockSpec(memory_space=pltpu.VMEM),
                pl.BlockSpec(memory_space=pl.ANY),
                pl.BlockSpec(memory_space=pl.ANY),
            ],
            out_specs=pl.BlockSpec(memory_space=pltpu.VMEM),
            scratch_shapes=scratch,
            compiler_params=pltpu.CompilerParams(collective_id=0, has_side_effects=True),
        )(pair_events, pair_counts, residuals[0], green_tensor, strain)

    in_specs = (
        P("sta", None, None, "vox"),
        P("sta", None, None, "vox"),
        P("sta", None),
        P("sta"),
        P("sta", None, None),
    )
    out_specs = P(("vox", "sta"))
    return jax.shard_map(body, mesh=mesh, in_specs=in_specs, out_specs=out_specs, check_vma=False)
```

```python
import functools

import jax
import jax.numpy as jnp
from jax import lax
from jax.experimental import pallas as pl
from jax.experimental.pallas import tpu as pltpu
from jax.sharding import PartitionSpec as P

LANES = 128
F32 = jnp.float32
BF16 = jnp.bfloat16


def kernel(
    n, events_ref, counts_ref, resid_ref, green_hbm, strain_hbm, out_ref,
    green, strain, packed_green, packed_strain, all_comb, all_green, all_strain, adjoint,
    load_sem, send_sem, recv_sem,
):
    me = lax.axis_index("sta")
    comps, nt, vox = green.shape
    local_events = strain.shape[0]
    slots = resid_ref.shape[0]
    width = vox // n
    per_tile = LANES // width
    full = comps // per_tile
    rest = comps % per_tile
    fit = min(per_tile // rest, local_events) if rest else 1
    blocks = nt // LANES

    def peer(d):
        pair = lax.rem(me // 2 + d // 2, n // 2)
        return 2 * pair + lax.rem(me + d, 2)

    order = list(range(n - 1, 0, -1))
    load_green = pltpu.make_async_copy(green_hbm.at[0], green, load_sem.at[0])
    load_strain = pltpu.make_async_copy(strain_hbm, strain, load_sem.at[1])
    load_green.start()
    load_strain.start()

    barrier = pltpu.get_barrier_semaphore()
    for d in order:
        pl.semaphore_signal(
            barrier, inc=1, device_id={"sta": peer(d)}, device_id_type=pl.DeviceIdType.MESH
        )

    def send(kind, src, dst, d):
        copy = pltpu.make_async_remote_copy(
            src_ref=src,
            dst_ref=dst.at[me],
            send_sem=send_sem.at[kind, d],
            recv_sem=recv_sem.at[kind, me],
            device_id={"sta": peer(d)},
            device_id_type=pl.DeviceIdType.MESH,
        )
        copy.start()
        return copy

    def wait_from(kind, dst, j):
        pltpu.make_async_remote_copy(
            src_ref=dst.at[j],
            dst_ref=dst.at[j],
            send_sem=send_sem.at[kind, 0],
            recv_sem=recv_sem.at[kind, j],
            device_id={"sta": j},
            device_id_type=pl.DeviceIdType.MESH,
        ).wait_recv()

    rows = lax.broadcasted_iota(jnp.int32, (all_comb.shape[1], nt), 0)
    comb = jnp.zeros((all_comb.shape[1], nt), F32)
    for p in range(slots):
        event = jnp.where(p < counts_ref[0], events_ref[0, p], -1)
        comb = comb + jnp.where(rows == event, resid_ref[p : p + 1, :], 0.0)
    all_comb[me] = comb

    lane = lax.broadcasted_iota(jnp.int32, (LANES, LANES), 0)
    column = lax.broadcasted_iota(jnp.int32, (LANES, LANES), 1)

    def pick(j, slot):
        inside = (column >= slot * width) & (column < (slot + 1) * width)
        return inside & (lane == column + (j - slot) * width)

    def as_matrix(masks):
        return jnp.concatenate([jnp.where(m, 1.0, 0.0).astype(BF16) for m in masks], axis=0)

    def gathered(tiles, matrix):
        wide = jnp.concatenate(tiles, axis=1)
        return jnp.dot(wide, matrix[: len(tiles) * LANES], preferred_element_type=F32).astype(BF16)

    def pack_green(j, masks, matrix, dst, index):
        for a in range(full):
            dst[index, a] = gathered([green[a * per_tile + k] for k in range(per_tile)], matrix)
        if rest:
            repeated = []
            for k in range(rest):
                hit = masks[k]
                for i in range(1, fit):
                    hit = hit | masks[i * rest + k]
                repeated.append(hit)
            dst[index, full] = gathered(
                [green[full * per_tile + k] for k in range(rest)], as_matrix(repeated)
            )

    def pack_strain(matrix, dst, index):
        tile = 0
        for e in range(local_events):
            for a in range(full):
                dst[index, tile] = gathered(
                    [strain[e, a * per_tile + k] for k in range(per_tile)], matrix
                )
                tile += 1
        if rest:
            for e in range(0, local_events, fit):
                dst[index, tile] = gathered(
                    [strain[e + i, full * per_tile + k] for i in range(fit) for k in range(rest)],
                    matrix,
                )
                tile += 1

    matrices = {}
    for d in order + [0]:
        j = peer(d)
        masks = [pick(j, slot) for slot in range(per_tile)]
        matrices[d] = (j, masks, as_matrix(masks))

    load_green.wait()
    copies = []
    pl.semaphore_wait(barrier, n - 1)
    for d in order:
        copies.append(send(0, all_comb.at[me], all_comb, d))
    waiting = None
    for d in order:
        pack_green(*matrices[d], packed_green, d)
        if waiting is not None:
            copies.append(send(1, packed_green.at[waiting], all_green, waiting))
        waiting = d
    pack_green(*matrices[0], all_green, me)
    copies.append(send(1, packed_green.at[waiting], all_green, waiting))
    load_strain.wait()
    waiting = None
    for d in order:
        pack_strain(matrices[d][2], packed_strain, d)
        if waiting is not None:
            copies.append(send(2, packed_strain.at[waiting], all_strain, waiting))
        waiting = d
    pack_strain(matrices[0][2], all_strain, me)
    copies.append(send(2, packed_strain.at[waiting], all_strain, waiting))

    for d in order:
        wait_from(0, all_comb, peer(d))
    for d in order:
        wait_from(1, all_green, peer(d))

    later = column >= lane
    nothing = jnp.zeros((LANES, LANES), BF16)
    tiles = all_green.shape[1]

    @pl.loop(0, all_comb.shape[1])
    def _(e):
        total = jnp.zeros((nt, tiles * LANES), F32)
        for s in range(n):
            wave = all_comb[s, pl.ds(e, 1), :]
            turned = []
            for k in range(blocks):
                piece = jnp.broadcast_to(wave[:, k * LANES : (k + 1) * LANES], (LANES, LANES))
                turned.append(pltpu.roll(piece, 0, 1, stride=1, stride_axis=0))
            diag = [
                jnp.where(later, turned[k], turned[k - 1] if k else 0.0).astype(BF16)
                for k in range(blocks)
            ]
            matrix = jnp.concatenate(
                [
                    jnp.concatenate([nothing] * i + diag[: blocks - i], axis=1)
                    for i in range(blocks)
                ],
                axis=0,
            )
            field = jnp.concatenate([all_green[s, t] for t in range(tiles)], axis=1)
            total = total + jnp.dot(matrix, field, preferred_element_type=F32)
        adjoint[e] = total

    spot = lax.broadcasted_iota(jnp.int32, (nt, LANES), 1)

    def meet(j):
        part = jnp.zeros((1, LANES), F32)
        tile = 0
        for e in range(local_events):
            for a in range(full):
                field = all_strain[j, tile].astype(F32)
                one = adjoint[j * local_events + e, :, a * LANES : (a + 1) * LANES]
                part = part + jnp.sum(field * one, axis=0, keepdims=True)
                tile += 1
        if rest:
            for e in range(0, local_events, fit):
                field = all_strain[j, tile].astype(F32)
                one = adjoint[j * local_events + e, :, full * LANES :]
                for i in range(1, fit):
                    other = adjoint[j * local_events + e + i, :, full * LANES :]
                    one = jnp.where(spot < i * rest * width, one, other)
                part = part + jnp.sum(
                    jnp.where(spot < fit * rest * width, field * one, 0.0), axis=0, keepdims=True
                )
                tile += 1
        return part

    answer = meet(me)
    for d in order:
        j = peer(d)
        wait_from(2, all_strain, j)
        answer = answer + meet(j)
    total = answer[:, :width]
    for k in range(1, per_tile):
        total = total + answer[:, k * width : (k + 1) * width]
    out_ref[...] = total[0]
    for copy in copies:
        copy.wait_send()


def square_kernel(
    events_hbm, counts_hbm, resid_hbm, green_hbm, strain_hbm, out_ref,
    events_ref, counts_ref, resid, green, strain,
    send_head, own_head, far_head, send_field, own_field, far_field,
    send_tail, own_tail, far_tail, send_bits, own_bits, far_bits, own_wide, far_wide,
    waves, rows_of, toeplitz, head_sum, tail_sum, far_head_sum, far_tail_sum, side_sum, load_sem, send_sem, recv_sem,
):
    me = lax.axis_index("sta")
    x, y = lax.rem(me, 2), me // 2
    odd = lax.rem(x + y, 2)
    beside = me + 1 - 2 * x
    above = lax.rem(me + 2, 4)
    first = beside + odd * (above - beside)
    second = above + odd * (beside - above)
    across = 3 - me
    comps, nt, vox = green.shape
    local_events = strain.shape[0]
    events = waves.shape[1]
    width = vox // 4
    per_tile = LANES // width
    rest = comps - per_tile
    half = nt // 2

    barrier = pltpu.get_barrier_semaphore()
    for target in (first, second):
        pl.semaphore_signal(
            barrier, inc=1, device_id={"sta": target}, device_id_type=pl.DeviceIdType.MESH
        )

    loads = {}
    for name, src, dst in (
        ("green", green_hbm.at[0], green),
        ("events", events_hbm, events_ref),
        ("counts", counts_hbm, counts_ref),
        ("resid", resid_hbm, resid),
        ("strain", strain_hbm, strain),
    ):
        loads[name] = pltpu.make_async_copy(src, dst, load_sem.at[len(loads)])
        loads[name].start()

    low_half, high_half = pl.ds(0, LANES), pl.ds(LANES, LANES)
    plan = {}
    for name, src, dst, target in (
        ("u0h", send_head.at[0], far_head.at[2], first),
        ("u2h", far_head.at[0], own_head.at[2], first),
        ("u3h", far_head.at[2], own_head.at[3], first),
        ("w1h", send_head.at[1], own_head.at[1], second),
        ("w0h", own_head.at[0], far_head.at[1], second),
        ("w4h", own_head.at[1], far_head.at[3], second),
        ("u0t", send_tail.at[0], far_tail.at[2], first),
        ("u2t", far_tail.at[0], own_tail.at[2], first),
        ("u3t", far_tail.at[2], own_tail.at[3], first),
        ("w1t", send_tail.at[1], own_tail.at[1], second),
        ("w0t", own_tail.at[0], far_tail.at[1], second),
        ("w4t", own_tail.at[1], far_tail.at[3], second),
        ("wave1", waves.at[0], waves.at[2], first),
        ("wave2", waves.at[0], waves.at[1], second),
        ("wave3", waves.at[2, :, low_half], waves.at[3, :, low_half], first),
        ("wave4", waves.at[1, :, high_half], waves.at[3, :, high_half], second),
        ("side", side_sum.at[0], side_sum.at[1], first),
        *(
            item
            for e in range(local_events)
            for item in (
                (f"u1h{e}", send_field.at[0, e], far_field.at[1, e], first),
                (f"w2h{e}", send_field.at[1, e], own_field.at[1, e], second),
                (f"u1t{e}", send_bits.at[0, e], far_bits.at[1, e], first),
                (f"w2t{e}", send_bits.at[1, e], own_bits.at[1, e], second),
            )
        ),
    ):
        plan[name] = pltpu.make_async_remote_copy(
            src_ref=src,
            dst_ref=dst,
            send_sem=send_sem.at[len(plan)],
            recv_sem=recv_sem.at[len(plan)],
            device_id={"sta": target},
            device_id_type=pl.DeviceIdType.MESH,
        )

    core = lax.rem(lax.axis_index("vox"), 2)

    def start(*names):
        for name in names:
            plan[name].start()

    def start_on(which, *names):
        @pl.when(core == which)
        def _():
            start(*names)

    def arrive(*names):
        for name in names:
            plan[name].wait_recv()

    each = range(local_events)
    lane = lax.broadcasted_iota(jnp.int32, (LANES, LANES), 0)
    column = lax.broadcasted_iota(jnp.int32, (LANES, LANES), 1)
    later = column >= lane
    low = column < LANES // 2

    def picker(j):
        parts = []
        for slot in range(per_tile):
            inside = (column >= slot * width) & (column < (slot + 1) * width)
            hit = inside & (lane == column + (j - slot) * width)
            parts.append(jnp.where(hit, 1.0, 0.0).astype(BF16))
        return jnp.concatenate(parts, axis=0)

    def wide_head(source):
        return jnp.concatenate([source[k] for k in range(per_tile)], axis=1)

    def wide_tail(source):
        return jnp.concatenate(
            [source[per_tile + k, h * half : (h + 1) * half] for h in range(2) for k in range(rest)],
            axis=1,
        )

    def pack(wides, pickers, *outs):
        wide = jnp.concatenate(wides, axis=0)
        both = jnp.dot(wide, pickers, preferred_element_type=F32).astype(BF16)
        at = 0
        for left, right in outs:
            size = left.shape[0]
            left[...] = both[at : at + size, :LANES]
            right[...] = both[at : at + size, LANES:]
            at += size

    def make_toeplitz(s):
        rows_of[...] = waves[s].astype(F32)

        for k in range(3 * local_events):
            owner = (me, first, second)[k // local_events]
            wave = rows_of[pl.ds(owner * local_events + k % local_events, 1), :]
            before = 0.0
            for b in range(2):
                piece = jnp.broadcast_to(wave[:, b * LANES : (b + 1) * LANES], (LANES, LANES))
                turned = pltpu.roll(piece, 0, 1, stride=1, stride_axis=0)
                toeplitz[k, s, b] = jnp.where(later, turned, before).astype(BF16)
                before = turned

    def widen(source, s, dst):
        piece = source[s].astype(F32)
        dst[s, :half] = source[s]
        dst[s, half:] = jnp.where(low, pltpu.roll(piece, LANES // 2, 1), 0.0).astype(BF16)

    nothing = jnp.zeros((half, half), BF16)

    def top(k, stations):
        return jnp.concatenate([toeplitz[k, s, b] for s in stations for b in range(2)], axis=1)

    def bottom(k, stations):
        return jnp.concatenate(
            [piece for s in stations for piece in (nothing, toeplitz[k, s, 0])], axis=1
        )

    def stack(fields, stations):
        return jnp.concatenate([fields[s] for s in stations], axis=0)

    def head_dot(ks, stations, field):
        matrix = jnp.concatenate([f(k, stations) for k in ks for f in (top, bottom)], axis=0)
        return jnp.dot(matrix, field, preferred_element_type=F32)

    def tail_dot(ks, stations, field):
        matrix = jnp.concatenate([top(k, stations) for k in ks], axis=0)
        return jnp.dot(matrix, field, preferred_element_type=F32)

    def met(field, adjoint):
        return jnp.sum(field.astype(F32) * adjoint, axis=0, keepdims=True)

    away = jnp.concatenate([picker(across), picker(second)], axis=1)
    loads["green"].wait()
    pack([wide_head(green)], away, (send_head.at[0], send_head.at[1]))
    pl.semaphore_wait(barrier, 2)
    start("u0h", "w1h")

    for name in ("events", "counts", "resid"):
        loads[name].wait()
    rows = lax.broadcasted_iota(jnp.int32, (events, nt), 0)
    comb = jnp.zeros((events, nt), F32)
    for p in range(resid.shape[1]):
        event = jnp.where(p < counts_ref[0], events_ref[0, p], -1)
        comb = comb + jnp.where(rows == event, resid[0, p : p + 1, :], 0.0)
    waves[0] = comb.astype(BF16)
    start("wave1", "wave2")

    pack([wide_tail(green)], away, (send_tail.at[0], send_tail.at[1]))
    start("u0t", "w1t")
    near = jnp.concatenate([picker(me), picker(first)], axis=1)
    pack(
        [wide_head(green), wide_tail(green)],
        near,
        (own_head.at[0], far_head.at[0]),
        (own_tail.at[0], far_tail.at[0]),
    )
    start("w0h", "w0t")
    loads["strain"].wait()
    pack(
        [f(strain.at[e]) for f in (wide_head, wide_tail) for e in each],
        away,
        *((send_field.at[0, e], send_field.at[1, e]) for e in each),
        *((send_bits.at[0, e], send_bits.at[1, e]) for e in each),
    )
    start("u1h0", "u1h1")
    arrive("wave1", "wave2")
    start("wave3", "wave4", "u1t0", "u1t1")
    arrive("w1h")
    start("w4h")
    arrive("w1t")
    start("w4t")
    start_on(0, "u2h", "w2h0", "w2h1")
    arrive("u0h")
    start_on(0, "u3h", "u2t", "w2t0", "w2t1")
    arrive("u0t")
    start_on(0, "u3t")
    pack(
        [f(strain.at[e]) for f in (wide_head, wide_tail) for e in each],
        near,
        *((own_field.at[0, e], far_field.at[0, e]) for e in each),
        *((own_bits.at[0, e], far_bits.at[0, e]) for e in each),
    )
    early, late = range(2), (3,)
    ours = range(2 * local_events)
    theirs = [*each, *range(2 * local_events, 3 * local_events)]

    def gather(ks, stations, heads, wides, heads_to, tails_to, fresh):
        field = jnp.concatenate([stack(heads, stations), stack(wides, stations)], axis=1)
        both = head_dot(ks, stations, field)
        for i in ours:
            head, tail = both[i * nt : (i + 1) * nt, :LANES], both[i * nt : i * nt + half, LANES:]
            heads_to[i] = head if fresh else heads_to[i] + head
            tails_to[i] = tail if fresh else tails_to[i] + tail

    make_toeplitz(0)
    make_toeplitz(2)
    widen(far_tail, 0, far_wide)
    widen(far_tail, 2, far_wide)
    gather(theirs, (0, 2), far_head, far_wide, far_head_sum, far_tail_sum, True)
    make_toeplitz(1)
    widen(own_tail, 0, own_wide)
    widen(own_tail, 1, own_wide)
    gather(ours, early, own_head, own_wide, head_sum, tail_sum, True)
    arrive("wave3", "wave4")
    make_toeplitz(3)
    arrive("w0h", "w0t")
    widen(far_tail, 1, far_wide)
    gather(theirs, (1,), far_head, far_wide, far_head_sum, far_tail_sum, False)
    start_on(1, "w2h0", "w2h1", "u2h", "u3h", "u2t", "w2t0", "w2t1", "u3t")
    arrive("w4h", "w4t")
    widen(far_tail, 3, far_wide)
    field = jnp.concatenate([far_head[3], far_wide[3]], axis=1)
    both = head_dot(theirs, late, field)
    for e in each:
        arrive(f"u1h{e}", f"u1t{e}")
    part = jnp.zeros((1, LANES), F32)
    for i in ours:
        side, e = i // local_events, i % local_events
        head, tail = both[i * nt : (i + 1) * nt, :LANES], both[i * nt : i * nt + half, LANES:]
        part = part + met(far_field[side, e], far_head_sum[i] + head)
        part = part + met(far_bits[side, e], far_tail_sum[i] + tail)
    side_sum[0] = part
    start("side")

    arrive("u2h")
    two = head_dot(ours, (2,), own_head[2])
    for k in ours:
        head_sum[k] += two[k * nt : (k + 1) * nt]
    arrive("u3h")
    three = head_dot(ours, late, own_head[3])
    for e in each:
        arrive(f"w2h{e}")
    part = jnp.zeros((1, LANES), F32)
    for k in ours:
        field = own_field[k // local_events, k % local_events]
        part = part + met(field, head_sum[k] + three[k * nt : (k + 1) * nt])
    arrive("u2t")
    widen(own_tail, 2, own_wide)
    two = tail_dot(ours, (2,), own_wide[2])
    for k in ours:
        tail_sum[k] += two[k * half : (k + 1) * half]
    arrive("u3t")
    widen(own_tail, 3, own_wide)
    three = tail_dot(ours, late, own_wide[3])
    for e in each:
        arrive(f"w2t{e}")
    for k in ours:
        field = own_bits[k // local_events, k % local_events]
        part = part + met(field, tail_sum[k] + three[k * half : (k + 1) * half])
    arrive("side")
    answer = part + side_sum[1]
    total = answer[:, :width]
    for k in range(1, per_tile):
        total = total + answer[:, k * width : (k + 1) * width]
    out_ref[...] = total[0]
    for copy in plan.values():
        copy.wait_send()


def solution(mesh):
    n = mesh.shape["sta"]

    def body(green_tensor, strain, pair_events, pair_counts, residuals):
        _, comps, nt, vox = green_tensor.shape
        local_events = strain.shape[0]
        width = vox // n
        per_tile = LANES // width
        full = comps // per_tile
        rest = comps % per_tile
        fit = min(per_tile // rest, local_events) if rest else 1
        green_tiles = full + (1 if rest else 0)
        strain_tiles = full * local_events + (local_events // fit if rest else 0)
        events = n * local_events
        square = n == 4 and nt == 2 * LANES and full == 1 and 2 * rest == per_tile
        if square:
            steps = square_kernel
            pairs = pair_events.shape[1]
            half = nt // 2
            copies = 17 + 4 * local_events
            scratch = [
                pltpu.SMEM((1, pairs), jnp.int32),
                pltpu.SMEM((1,), jnp.int32),
                pltpu.VMEM((1, pairs, nt), F32),
                pltpu.VMEM((comps, nt, vox), BF16),
                pltpu.VMEM((local_events, comps, nt, vox), BF16),
                *(pltpu.VMEM((k, nt, LANES), BF16) for k in (2, 4, 4)),
                *(pltpu.VMEM((2, local_events, nt, LANES), BF16) for _ in range(3)),
                *(pltpu.VMEM((k, half, LANES), BF16) for k in (2, 4, 4)),
                *(pltpu.VMEM((2, local_events, half, LANES), BF16) for _ in range(3)),
                *(pltpu.VMEM((4, nt, LANES), BF16) for _ in range(2)),
                pltpu.VMEM((4, events, nt), BF16),
                pltpu.VMEM((events, nt), F32),
                pltpu.VMEM((3 * local_events, 4, 2, half, half), BF16),
                pltpu.VMEM((2 * local_events, nt, LANES), F32),
                pltpu.VMEM((2 * local_events, half, LANES), F32),
                pltpu.VMEM((2 * local_events, nt, LANES), F32),
                pltpu.VMEM((2 * local_events, half, LANES), F32),
                pltpu.VMEM((2, 1, LANES), F32),
                pltpu.SemaphoreType.DMA((5,)),
                pltpu.SemaphoreType.DMA((copies,)),
                pltpu.SemaphoreType.DMA((copies,)),
            ]
        else:
            steps = functools.partial(kernel, n)
            scratch = [
                pltpu.VMEM((comps, nt, vox), BF16),
                pltpu.VMEM((local_events, comps, nt, vox), BF16),
                pltpu.VMEM((n, green_tiles, nt, LANES), BF16),
                pltpu.VMEM((n, strain_tiles, nt, LANES), BF16),
                pltpu.VMEM((n, events, nt), F32),
                pltpu.VMEM((n, green_tiles, nt, LANES), BF16),
                pltpu.VMEM((n, strain_tiles, nt, LANES), BF16),
                pltpu.VMEM((events, nt, green_tiles * LANES), F32),
                pltpu.SemaphoreType.DMA((2,)),
                pltpu.SemaphoreType.DMA((3, n)),
                pltpu.SemaphoreType.DMA((3, n)),
            ]
        if square:
            return pl.pallas_call(
                steps,
                out_shape=pltpu.VMEM((width,), F32),
                in_specs=[pl.BlockSpec(memory_space=pl.ANY)] * 5,
                out_specs=pl.BlockSpec(memory_space=pltpu.VMEM),
                scratch_shapes=scratch,
                compiler_params=pltpu.CompilerParams(collective_id=0, has_side_effects=True),
            )(pair_events, pair_counts, residuals, green_tensor, strain)
        return pl.pallas_call(
            steps,
            out_shape=jax.ShapeDtypeStruct((width,), F32),
            in_specs=[
                pl.BlockSpec(memory_space=pltpu.SMEM),
                pl.BlockSpec(memory_space=pltpu.SMEM),
                pl.BlockSpec(memory_space=pltpu.VMEM),
                pl.BlockSpec(memory_space=pl.ANY),
                pl.BlockSpec(memory_space=pl.ANY),
            ],
            out_specs=pl.BlockSpec(memory_space=pltpu.VMEM),
            scratch_shapes=scratch,
            compiler_params=pltpu.CompilerParams(collective_id=0, has_side_effects=True),
        )(pair_events, pair_counts, residuals[0], green_tensor, strain)

    in_specs = (
        P("sta", None, None, "vox"),
        P("sta", None, None, "vox"),
        P("sta", None),
        P("sta"),
        P("sta", None, None),
    )
    out_specs = P(("vox", "sta"))
    return jax.shard_map(body, mesh=mesh, in_specs=in_specs, out_specs=out_specs, check_vma=False)
```

```python
import functools

import jax
import jax.numpy as jnp
from jax import lax
from jax.experimental import pallas as pl
from jax.experimental.pallas import tpu as pltpu
from jax.sharding import PartitionSpec as P

LANES = 128
F32 = jnp.float32
BF16 = jnp.bfloat16


def kernel(
    n, events_ref, counts_ref, resid_ref, green_hbm, strain_hbm, out_ref,
    green, strain, packed_green, packed_strain, all_comb, all_green, all_strain, adjoint,
    load_sem, send_sem, recv_sem,
):
    me = lax.axis_index("sta")
    comps, nt, vox = green.shape
    local_events = strain.shape[0]
    slots = resid_ref.shape[0]
    width = vox // n
    per_tile = LANES // width
    full = comps // per_tile
    rest = comps % per_tile
    fit = min(per_tile // rest, local_events) if rest else 1
    blocks = nt // LANES

    def peer(d):
        pair = lax.rem(me // 2 + d // 2, n // 2)
        return 2 * pair + lax.rem(me + d, 2)

    order = list(range(n - 1, 0, -1))
    load_green = pltpu.make_async_copy(green_hbm.at[0], green, load_sem.at[0])
    load_strain = pltpu.make_async_copy(strain_hbm, strain, load_sem.at[1])
    load_green.start()
    load_strain.start()

    barrier = pltpu.get_barrier_semaphore()
    for d in order:
        pl.semaphore_signal(
            barrier, inc=1, device_id={"sta": peer(d)}, device_id_type=pl.DeviceIdType.MESH
        )

    def send(kind, src, dst, d):
        copy = pltpu.make_async_remote_copy(
            src_ref=src,
            dst_ref=dst.at[me],
            send_sem=send_sem.at[kind, d],
            recv_sem=recv_sem.at[kind, me],
            device_id={"sta": peer(d)},
            device_id_type=pl.DeviceIdType.MESH,
        )
        copy.start()
        return copy

    def wait_from(kind, dst, j):
        pltpu.make_async_remote_copy(
            src_ref=dst.at[j],
            dst_ref=dst.at[j],
            send_sem=send_sem.at[kind, 0],
            recv_sem=recv_sem.at[kind, j],
            device_id={"sta": j},
            device_id_type=pl.DeviceIdType.MESH,
        ).wait_recv()

    rows = lax.broadcasted_iota(jnp.int32, (all_comb.shape[1], nt), 0)
    comb = jnp.zeros((all_comb.shape[1], nt), F32)
    for p in range(slots):
        event = jnp.where(p < counts_ref[0], events_ref[0, p], -1)
        comb = comb + jnp.where(rows == event, resid_ref[p : p + 1, :], 0.0)
    all_comb[me] = comb

    lane = lax.broadcasted_iota(jnp.int32, (LANES, LANES), 0)
    column = lax.broadcasted_iota(jnp.int32, (LANES, LANES), 1)

    def pick(j, slot):
        inside = (column >= slot * width) & (column < (slot + 1) * width)
        return inside & (lane == column + (j - slot) * width)

    def as_matrix(masks):
        return jnp.concatenate([jnp.where(m, 1.0, 0.0).astype(BF16) for m in masks], axis=0)

    def gathered(tiles, matrix):
        wide = jnp.concatenate(tiles, axis=1)
        return jnp.dot(wide, matrix[: len(tiles) * LANES], preferred_element_type=F32).astype(BF16)

    def pack_green(j, masks, matrix, dst, index):
        for a in range(full):
            dst[index, a] = gathered([green[a * per_tile + k] for k in range(per_tile)], matrix)
        if rest:
            repeated = []
            for k in range(rest):
                hit = masks[k]
                for i in range(1, fit):
                    hit = hit | masks[i * rest + k]
                repeated.append(hit)
            dst[index, full] = gathered(
                [green[full * per_tile + k] for k in range(rest)], as_matrix(repeated)
            )

    def pack_strain(matrix, dst, index):
        tile = 0
        for e in range(local_events):
            for a in range(full):
                dst[index, tile] = gathered(
                    [strain[e, a * per_tile + k] for k in range(per_tile)], matrix
                )
                tile += 1
        if rest:
            for e in range(0, local_events, fit):
                dst[index, tile] = gathered(
                    [strain[e + i, full * per_tile + k] for i in range(fit) for k in range(rest)],
                    matrix,
                )
                tile += 1

    matrices = {}
    for d in order + [0]:
        j = peer(d)
        masks = [pick(j, slot) for slot in range(per_tile)]
        matrices[d] = (j, masks, as_matrix(masks))

    load_green.wait()
    copies = []
    pl.semaphore_wait(barrier, n - 1)
    for d in order:
        copies.append(send(0, all_comb.at[me], all_comb, d))
    waiting = None
    for d in order:
        pack_green(*matrices[d], packed_green, d)
        if waiting is not None:
            copies.append(send(1, packed_green.at[waiting], all_green, waiting))
        waiting = d
    pack_green(*matrices[0], all_green, me)
    copies.append(send(1, packed_green.at[waiting], all_green, waiting))
    load_strain.wait()
    waiting = None
    for d in order:
        pack_strain(matrices[d][2], packed_strain, d)
        if waiting is not None:
            copies.append(send(2, packed_strain.at[waiting], all_strain, waiting))
        waiting = d
    pack_strain(matrices[0][2], all_strain, me)
    copies.append(send(2, packed_strain.at[waiting], all_strain, waiting))

    for d in order:
        wait_from(0, all_comb, peer(d))
    for d in order:
        wait_from(1, all_green, peer(d))

    later = column >= lane
    nothing = jnp.zeros((LANES, LANES), BF16)
    tiles = all_green.shape[1]

    @pl.loop(0, all_comb.shape[1])
    def _(e):
        total = jnp.zeros((nt, tiles * LANES), F32)
        for s in range(n):
            wave = all_comb[s, pl.ds(e, 1), :]
            turned = []
            for k in range(blocks):
                piece = jnp.broadcast_to(wave[:, k * LANES : (k + 1) * LANES], (LANES, LANES))
                turned.append(pltpu.roll(piece, 0, 1, stride=1, stride_axis=0))
            diag = [
                jnp.where(later, turned[k], turned[k - 1] if k else 0.0).astype(BF16)
                for k in range(blocks)
            ]
            matrix = jnp.concatenate(
                [
                    jnp.concatenate([nothing] * i + diag[: blocks - i], axis=1)
                    for i in range(blocks)
                ],
                axis=0,
            )
            field = jnp.concatenate([all_green[s, t] for t in range(tiles)], axis=1)
            total = total + jnp.dot(matrix, field, preferred_element_type=F32)
        adjoint[e] = total

    spot = lax.broadcasted_iota(jnp.int32, (nt, LANES), 1)

    def meet(j):
        part = jnp.zeros((1, LANES), F32)
        tile = 0
        for e in range(local_events):
            for a in range(full):
                field = all_strain[j, tile].astype(F32)
                one = adjoint[j * local_events + e, :, a * LANES : (a + 1) * LANES]
                part = part + jnp.sum(field * one, axis=0, keepdims=True)
                tile += 1
        if rest:
            for e in range(0, local_events, fit):
                field = all_strain[j, tile].astype(F32)
                one = adjoint[j * local_events + e, :, full * LANES :]
                for i in range(1, fit):
                    other = adjoint[j * local_events + e + i, :, full * LANES :]
                    one = jnp.where(spot < i * rest * width, one, other)
                part = part + jnp.sum(
                    jnp.where(spot < fit * rest * width, field * one, 0.0), axis=0, keepdims=True
                )
                tile += 1
        return part

    answer = meet(me)
    for d in order:
        j = peer(d)
        wait_from(2, all_strain, j)
        answer = answer + meet(j)
    total = answer[:, :width]
    for k in range(1, per_tile):
        total = total + answer[:, k * width : (k + 1) * width]
    out_ref[...] = total[0]
    for copy in copies:
        copy.wait_send()


def square_kernel(
    events_hbm, counts_hbm, resid_hbm, green_hbm, strain_hbm, out_ref,
    events_ref, counts_ref, resid, green, strain,
    send_head, own_head, far_head, send_field, own_field, far_field,
    send_tail, own_tail, far_tail, send_bits, own_bits, far_bits, own_wide, far_wide,
    waves, rows_of, toeplitz, head_sum, tail_sum, far_head_sum, far_tail_sum, side_sum, load_sem, send_sem, recv_sem,
):
    me = lax.axis_index("sta")
    x, y = lax.rem(me, 2), me // 2
    odd = lax.rem(x + y, 2)
    beside = me + 1 - 2 * x
    above = lax.rem(me + 2, 4)
    first = beside + odd * (above - beside)
    second = above + odd * (beside - above)
    across = 3 - me
    comps, nt, vox = green.shape
    local_events = strain.shape[0]
    events = waves.shape[1]
    width = vox // 4
    per_tile = LANES // width
    rest = comps - per_tile
    half = nt // 2

    barrier = pltpu.get_barrier_semaphore()
    for target in (first, second):
        pl.semaphore_signal(
            barrier, inc=1, device_id={"sta": target}, device_id_type=pl.DeviceIdType.MESH
        )

    loads = {}
    for name, src, dst in (
        ("green", green_hbm.at[0], green),
        ("events", events_hbm, events_ref),
        ("counts", counts_hbm, counts_ref),
        ("resid", resid_hbm, resid),
        ("strain", strain_hbm, strain),
    ):
        loads[name] = pltpu.make_async_copy(src, dst, load_sem.at[len(loads)])
        loads[name].start()

    low_half, high_half = pl.ds(0, LANES), pl.ds(LANES, LANES)
    plan = {}
    for name, src, dst, target in (
        ("u0h", send_head.at[0], far_head.at[2], first),
        ("u2h", far_head.at[0], own_head.at[2], first),
        ("u3h", far_head.at[2], own_head.at[3], first),
        ("w1h", send_head.at[1], own_head.at[1], second),
        ("w0h", own_head.at[0], far_head.at[1], second),
        ("w4h", own_head.at[1], far_head.at[3], second),
        ("u0t", send_tail.at[0], far_tail.at[2], first),
        ("u2t", far_tail.at[0], own_tail.at[2], first),
        ("u3t", far_tail.at[2], own_tail.at[3], first),
        ("w1t", send_tail.at[1], own_tail.at[1], second),
        ("w0t", own_tail.at[0], far_tail.at[1], second),
        ("w4t", own_tail.at[1], far_tail.at[3], second),
        ("wave1", waves.at[0], waves.at[2], first),
        ("wave2", waves.at[0], waves.at[1], second),
        ("wave3", waves.at[2, :, low_half], waves.at[3, :, low_half], first),
        ("wave4", waves.at[1, :, high_half], waves.at[3, :, high_half], second),
        ("side", side_sum.at[0], side_sum.at[1], first),
        *(
            item
            for e in range(local_events)
            for item in (
                (f"u1h{e}", send_field.at[0, e], far_field.at[1, e], first),
                (f"w2h{e}", send_field.at[1, e], own_field.at[1, e], second),
                (f"u1t{e}", send_bits.at[0, e], far_bits.at[1, e], first),
                (f"w2t{e}", send_bits.at[1, e], own_bits.at[1, e], second),
            )
        ),
    ):
        plan[name] = pltpu.make_async_remote_copy(
            src_ref=src,
            dst_ref=dst,
            send_sem=send_sem.at[len(plan)],
            recv_sem=recv_sem.at[len(plan)],
            device_id={"sta": target},
            device_id_type=pl.DeviceIdType.MESH,
        )

    core = lax.rem(lax.axis_index("vox"), 2)

    def start(*names):
        for name in names:
            plan[name].start()

    def start_on(which, *names):
        @pl.when(core == which)
        def _():
            start(*names)

    def arrive(*names):
        for name in names:
            plan[name].wait_recv()

    each = range(local_events)
    lane = lax.broadcasted_iota(jnp.int32, (LANES, LANES), 0)
    column = lax.broadcasted_iota(jnp.int32, (LANES, LANES), 1)
    later = column >= lane
    low = column < LANES // 2

    def picker(j):
        parts = []
        for slot in range(per_tile):
            inside = (column >= slot * width) & (column < (slot + 1) * width)
            hit = inside & (lane == column + (j - slot) * width)
            parts.append(jnp.where(hit, 1.0, 0.0).astype(BF16))
        return jnp.concatenate(parts, axis=0)

    def wide_head(source):
        return jnp.concatenate([source[k] for k in range(per_tile)], axis=1)

    def wide_tail(source):
        return jnp.concatenate(
            [source[per_tile + k, h * half : (h + 1) * half] for h in range(2) for k in range(rest)],
            axis=1,
        )

    def pack(wides, pickers, *outs):
        wide = jnp.concatenate(wides, axis=0)
        both = jnp.dot(wide, pickers, preferred_element_type=F32).astype(BF16)
        at = 0
        for left, right in outs:
            size = left.shape[0]
            left[...] = both[at : at + size, :LANES]
            right[...] = both[at : at + size, LANES:]
            at += size

    def make_toeplitz(s):
        rows_of[...] = waves[s].astype(F32)

        for k in range(3 * local_events):
            owner = (me, first, second)[k // local_events]
            wave = rows_of[pl.ds(owner * local_events + k % local_events, 1), :]
            before = 0.0
            for b in range(2):
                piece = jnp.broadcast_to(wave[:, b * LANES : (b + 1) * LANES], (LANES, LANES))
                turned = pltpu.roll(piece, 0, 1, stride=1, stride_axis=0)
                toeplitz[k, s, b] = jnp.where(later, turned, before).astype(BF16)
                before = turned

    def widen(source, s, dst):
        piece = source[s].astype(F32)
        dst[s, :half] = source[s]
        dst[s, half:] = jnp.where(low, pltpu.roll(piece, LANES // 2, 1), 0.0).astype(BF16)

    nothing = jnp.zeros((half, half), BF16)

    def top(k, stations):
        return jnp.concatenate([toeplitz[k, s, b] for s in stations for b in range(2)], axis=1)

    def bottom(k, stations):
        return jnp.concatenate(
            [piece for s in stations for piece in (nothing, toeplitz[k, s, 0])], axis=1
        )

    def stack(fields, stations):
        return jnp.concatenate([fields[s] for s in stations], axis=0)

    def head_dot(ks, stations, field):
        matrix = jnp.concatenate([f(k, stations) for k in ks for f in (top, bottom)], axis=0)
        return jnp.dot(matrix, field, preferred_element_type=F32)

    def tail_dot(ks, stations, field):
        matrix = jnp.concatenate([top(k, stations) for k in ks], axis=0)
        return jnp.dot(matrix, field, preferred_element_type=F32)

    def met(field, adjoint):
        return jnp.sum(field.astype(F32) * adjoint, axis=0, keepdims=True)

    away = jnp.concatenate([picker(across), picker(second)], axis=1)
    loads["green"].wait()
    pack([wide_head(green)], away, (send_head.at[0], send_head.at[1]))
    pl.semaphore_wait(barrier, 2)
    start("u0h", "w1h")

    for name in ("events", "counts", "resid"):
        loads[name].wait()
    rows = lax.broadcasted_iota(jnp.int32, (events, nt), 0)
    comb = jnp.zeros((events, nt), F32)
    for p in range(resid.shape[1]):
        event = jnp.where(p < counts_ref[0], events_ref[0, p], -1)
        comb = comb + jnp.where(rows == event, resid[0, p : p + 1, :], 0.0)
    waves[0] = comb.astype(BF16)
    start("wave1", "wave2")

    pack([wide_tail(green)], away, (send_tail.at[0], send_tail.at[1]))
    start("u0t", "w1t")
    near = jnp.concatenate([picker(me), picker(first)], axis=1)
    pack(
        [wide_head(green), wide_tail(green)],
        near,
        (own_head.at[0], far_head.at[0]),
        (own_tail.at[0], far_tail.at[0]),
    )
    start("w0h")
    loads["strain"].wait()
    pack(
        [f(strain.at[e]) for f in (wide_head, wide_tail) for e in each],
        away,
        *((send_field.at[0, e], send_field.at[1, e]) for e in each),
        *((send_bits.at[0, e], send_bits.at[1, e]) for e in each),
    )
    start("u1h0", "u1h1")
    arrive("w1h")
    start("w4h", "w0t")
    arrive("wave1", "wave2")
    start("wave3", "wave4", "u1t0", "u1t1")
    arrive("w1t")
    start("w4t")
    start_on(0, "u2h", "w2h0", "w2h1")
    arrive("u0h")
    start_on(0, "u3h", "u2t", "w2t0", "w2t1")
    arrive("u0t")
    start_on(0, "u3t")
    pack(
        [f(strain.at[e]) for f in (wide_head, wide_tail) for e in each],
        near,
        *((own_field.at[0, e], far_field.at[0, e]) for e in each),
        *((own_bits.at[0, e], far_bits.at[0, e]) for e in each),
    )
    early, late = range(2), (3,)
    ours = range(2 * local_events)
    theirs = [*each, *range(2 * local_events, 3 * local_events)]

    def gather(ks, stations, heads, wides, heads_to, tails_to, fresh):
        field = jnp.concatenate([stack(heads, stations), stack(wides, stations)], axis=1)
        both = head_dot(ks, stations, field)
        for i in ours:
            head, tail = both[i * nt : (i + 1) * nt, :LANES], both[i * nt : i * nt + half, LANES:]
            heads_to[i] = head if fresh else heads_to[i] + head
            tails_to[i] = tail if fresh else tails_to[i] + tail

    make_toeplitz(0)
    make_toeplitz(2)
    widen(far_tail, 0, far_wide)
    widen(far_tail, 2, far_wide)
    gather(theirs, (0, 2), far_head, far_wide, far_head_sum, far_tail_sum, True)
    make_toeplitz(1)
    widen(own_tail, 0, own_wide)
    widen(own_tail, 1, own_wide)
    gather(ours, early, own_head, own_wide, head_sum, tail_sum, True)
    arrive("wave3", "wave4")
    make_toeplitz(3)
    arrive("w0h", "w0t")
    widen(far_tail, 1, far_wide)
    gather(theirs, (1,), far_head, far_wide, far_head_sum, far_tail_sum, False)
    start_on(1, "w2h0", "w2h1", "u2h", "u3h", "u2t", "w2t0", "w2t1", "u3t")
    arrive("w4h", "w4t")
    widen(far_tail, 3, far_wide)
    field = jnp.concatenate([far_head[3], far_wide[3]], axis=1)
    both = head_dot(theirs, late, field)
    for e in each:
        arrive(f"u1h{e}", f"u1t{e}")
    part = jnp.zeros((1, LANES), F32)
    for i in ours:
        side, e = i // local_events, i % local_events
        head, tail = both[i * nt : (i + 1) * nt, :LANES], both[i * nt : i * nt + half, LANES:]
        part = part + met(far_field[side, e], far_head_sum[i] + head)
        part = part + met(far_bits[side, e], far_tail_sum[i] + tail)
    side_sum[0] = part
    start("side")

    arrive("u2h")
    two = head_dot(ours, (2,), own_head[2])
    for k in ours:
        head_sum[k] += two[k * nt : (k + 1) * nt]
    arrive("u3h")
    three = head_dot(ours, late, own_head[3])
    for e in each:
        arrive(f"w2h{e}")
    part = jnp.zeros((1, LANES), F32)
    for k in ours:
        field = own_field[k // local_events, k % local_events]
        part = part + met(field, head_sum[k] + three[k * nt : (k + 1) * nt])
    arrive("u2t")
    widen(own_tail, 2, own_wide)
    two = tail_dot(ours, (2,), own_wide[2])
    for k in ours:
        tail_sum[k] += two[k * half : (k + 1) * half]
    arrive("u3t")
    widen(own_tail, 3, own_wide)
    three = tail_dot(ours, late, own_wide[3])
    for e in each:
        arrive(f"w2t{e}")
    for k in ours:
        field = own_bits[k // local_events, k % local_events]
        part = part + met(field, tail_sum[k] + three[k * half : (k + 1) * half])
    arrive("side")
    answer = part + side_sum[1]
    total = answer[:, :width]
    for k in range(1, per_tile):
        total = total + answer[:, k * width : (k + 1) * width]
    out_ref[...] = total[0]
    for copy in plan.values():
        copy.wait_send()


def solution(mesh):
    n = mesh.shape["sta"]

    def body(green_tensor, strain, pair_events, pair_counts, residuals):
        _, comps, nt, vox = green_tensor.shape
        local_events = strain.shape[0]
        width = vox // n
        per_tile = LANES // width
        full = comps // per_tile
        rest = comps % per_tile
        fit = min(per_tile // rest, local_events) if rest else 1
        green_tiles = full + (1 if rest else 0)
        strain_tiles = full * local_events + (local_events // fit if rest else 0)
        events = n * local_events
        square = n == 4 and nt == 2 * LANES and full == 1 and 2 * rest == per_tile
        if square:
            steps = square_kernel
            pairs = pair_events.shape[1]
            half = nt // 2
            copies = 17 + 4 * local_events
            scratch = [
                pltpu.SMEM((1, pairs), jnp.int32),
                pltpu.SMEM((1,), jnp.int32),
                pltpu.VMEM((1, pairs, nt), F32),
                pltpu.VMEM((comps, nt, vox), BF16),
                pltpu.VMEM((local_events, comps, nt, vox), BF16),
                *(pltpu.VMEM((k, nt, LANES), BF16) for k in (2, 4, 4)),
                *(pltpu.VMEM((2, local_events, nt, LANES), BF16) for _ in range(3)),
                *(pltpu.VMEM((k, half, LANES), BF16) for k in (2, 4, 4)),
                *(pltpu.VMEM((2, local_events, half, LANES), BF16) for _ in range(3)),
                *(pltpu.VMEM((4, nt, LANES), BF16) for _ in range(2)),
                pltpu.VMEM((4, events, nt), BF16),
                pltpu.VMEM((events, nt), F32),
                pltpu.VMEM((3 * local_events, 4, 2, half, half), BF16),
                pltpu.VMEM((2 * local_events, nt, LANES), F32),
                pltpu.VMEM((2 * local_events, half, LANES), F32),
                pltpu.VMEM((2 * local_events, nt, LANES), F32),
                pltpu.VMEM((2 * local_events, half, LANES), F32),
                pltpu.VMEM((2, 1, LANES), F32),
                pltpu.SemaphoreType.DMA((5,)),
                pltpu.SemaphoreType.DMA((copies,)),
                pltpu.SemaphoreType.DMA((copies,)),
            ]
        else:
            steps = functools.partial(kernel, n)
            scratch = [
                pltpu.VMEM((comps, nt, vox), BF16),
                pltpu.VMEM((local_events, comps, nt, vox), BF16),
                pltpu.VMEM((n, green_tiles, nt, LANES), BF16),
                pltpu.VMEM((n, strain_tiles, nt, LANES), BF16),
                pltpu.VMEM((n, events, nt), F32),
                pltpu.VMEM((n, green_tiles, nt, LANES), BF16),
                pltpu.VMEM((n, strain_tiles, nt, LANES), BF16),
                pltpu.VMEM((events, nt, green_tiles * LANES), F32),
                pltpu.SemaphoreType.DMA((2,)),
                pltpu.SemaphoreType.DMA((3, n)),
                pltpu.SemaphoreType.DMA((3, n)),
            ]
        if square:
            return pl.pallas_call(
                steps,
                out_shape=pltpu.VMEM((width,), F32),
                in_specs=[pl.BlockSpec(memory_space=pl.ANY)] * 5,
                out_specs=pl.BlockSpec(memory_space=pltpu.VMEM),
                scratch_shapes=scratch,
                compiler_params=pltpu.CompilerParams(collective_id=0, has_side_effects=True),
            )(pair_events, pair_counts, residuals, green_tensor, strain)
        return pl.pallas_call(
            steps,
            out_shape=jax.ShapeDtypeStruct((width,), F32),
            in_specs=[
                pl.BlockSpec(memory_space=pltpu.SMEM),
                pl.BlockSpec(memory_space=pltpu.SMEM),
                pl.BlockSpec(memory_space=pltpu.VMEM),
                pl.BlockSpec(memory_space=pl.ANY),
                pl.BlockSpec(memory_space=pl.ANY),
            ],
            out_specs=pl.BlockSpec(memory_space=pltpu.VMEM),
            scratch_shapes=scratch,
            compiler_params=pltpu.CompilerParams(collective_id=0, has_side_effects=True),
        )(pair_events, pair_counts, residuals[0], green_tensor, strain)

    in_specs = (
        P("sta", None, None, "vox"),
        P("sta", None, None, "vox"),
        P("sta", None),
        P("sta"),
        P("sta", None, None),
    )
    out_specs = P(("vox", "sta"))
    return jax.shard_map(body, mesh=mesh, in_specs=in_specs, out_specs=out_specs, check_vma=False)
```
